32 devices in a mesh: px: 8 (over z, y), py: 4 (over x, core).
Axes of the slice: x: 2, y: 2, z: 4, core: 2. Of those that a mesh axis runs over, the one named last changes fastest.
Arguments:
- mode_field: float32 [64, 512, 1024], P(None, 'px', 'py'), may hold values from -1 to 1
- forcing: float32 [64, 512, 1024], P(None, 'px', 'py'), may hold values from -8 to 8
- visc_base: float32 [64, 1024, 512], P('py', 'px'), may hold values from 0.1 to 3
- depth_inverse: float32 [1024, 64, 64], P('py'), may hold values from -1 to 2, as said below
Outputs:
- mode_field_out: float32 [64, 512, 1024], P(None, 'px', 'py')
- residual_norms: float32 [2], replicated
The draws below stay inside these ranges and needn't reach their ends.
Inputs may be any that keep to these rules, and one draw needn't show every extreme that they name: `depth_inverse`: each matrix has its diagonal between 0.5 and 1.5 and off-diagonal entries of magnitude at most 0.4 / sqrt(64).
All inputs are finite; a program needn't handle non-finite values.
Results may differ from the reference program's by a relative error of at most 0.0001.
Values sent between devices are 32-bit elements; how exact they have to be, the bound alone decides.
A program may use at most 128 MiB of HBM per device.

```python
import math
import jax
import jax.numpy as jnp
from jax import lax

Z = 64
NX = 1024
NY = 512
ITERS = 2


def draw_depth_inverse(key, part):
    first = jax.random.fold_in(key, 11)
    second = jax.random.fold_in(key, 12)
    spread = 0.4 / math.sqrt(Z)
    offdiag = jax.random.uniform(first, (NX, Z, Z), jnp.float32, -spread, spread)
    diagonal = jax.random.uniform(second, (NX, Z), jnp.float32, 0.5, 1.5)
    identity = jnp.eye(Z, dtype=jnp.float32)
    return offdiag * (1.0 - identity) + diagonal[:, :, None] * identity


def block_levels(stream_key, dims, shards, low, largest):
    loudness = 1.0
    for axis_at, parts in shards:
        steps = jax.random.uniform(jax.random.fold_in(jax.random.fold_in(stream_key, 6), axis_at), (parts,), jnp.float32, low / len(shards), largest / len(shards))
        loudness = loudness * jnp.repeat(jnp.exp(steps), dims[axis_at] // parts).reshape((-1,) + (1,) * (len(dims) - 1 - axis_at))
    return loudness


def gaussian(key, extent, deviation, reach, cuts=(), kind=jnp.bfloat16):
    result = jax.random.normal(key, extent, jnp.float32) * deviation
    if len(cuts) > 0:
        result = block_levels(key, extent, cuts, -0.22, 0.18) * result
    return jnp.clip(result, min=-reach, max=reach).astype(kind)


def setup_inputs(seed: int = 0) -> dict:
    splits = jax.random.split(jax.random.key(seed), 5)
    return {
        "mode_field": gaussian(splits[0], (Z, NY, NX), 0.125, 1.0, ((1, 8), (2, 4)), jnp.float32),
        "forcing": gaussian(splits[1], (Z, NY, NX), 1.0, 8.0, ((1, 8), (2, 4)), jnp.float32),
        "visc_base": jnp.clip(jnp.exp(math.log(3.0) - 3.4011974 * jax.random.uniform(splits[2], (Z, NX, NY), jnp.float32) ** block_levels(splits[2], (Z, NX, NY), ((0, 4), (1, 8)), -0.2, 0.2)), 0.1, 3.0),
        "depth_inverse": draw_depth_inverse(jax.random.fold_in(splits[4], 71), 0),
    }


def depth_tables(count):
    index = jnp.arange(count, dtype=jnp.float32)
    angle = jnp.pi * index[:, None] * index[None, :] / (count - 1)
    ends = jnp.where((index == 0) | (index == count - 1), 2.0, 1.0)
    forward = jnp.cos(angle)
    backward = 2.0 / (count - 1) * jnp.cos(angle) / (ends[:, None] * ends[None, :])
    return (forward, backward)

def hartley_axis(values, axis):
    spectrum = jnp.fft.fft(values, axis=axis)
    return (jnp.real(spectrum) - jnp.imag(spectrum)) / math.sqrt(values.shape[axis])

def wavenumber(count):
    index = jnp.arange(count, dtype=jnp.int32)
    folded = jnp.minimum(index, count - index).astype(jnp.float32)
    scaled = 2.0 * jnp.pi * folded / count
    return scaled * scaled

def reference(mode_field, forcing, visc_base, depth_inverse):
    forward, backward = depth_tables(Z)
    lateral = wavenumber(NY)[:, None] + wavenumber(NX)[None, :]
    field = mode_field
    norms = []
    for sweep in range(ITERS):
        points = jnp.einsum('jm,myx->jyx', forward, field, precision=lax.Precision.HIGHEST)
        physical = jnp.transpose(hartley_axis(hartley_axis(points, 2), 1), (0, 2, 1))
        stress = visc_base * jnp.power(1.0 + physical * physical, -1.0 / 3.0) * physical
        spectral = hartley_axis(hartley_axis(jnp.transpose(stress, (0, 2, 1)), 1), 2)
        viscous = jnp.einsum('mj,jyx->myx', backward, spectral, precision=lax.Precision.HIGHEST)
        residual = forcing - (lateral * field + viscous)
        norms.append(jnp.mean(residual * residual))
        correction = jnp.einsum('xmn,nyx->myx', depth_inverse, residual, precision=lax.Precision.HIGHEST)
        field = field + correction / (1.0 + lateral)
    return (field, jnp.stack(norms))
```

```python
import functools
import math

import jax
import jax.numpy as jnp
import numpy as np
from jax import lax
from jax.experimental import pallas as pl
from jax.experimental.pallas import tpu as pltpu
from jax.sharding import PartitionSpec as P

ITERS = 2
MESH = pl.DeviceIdType.MESH
HIGH = lax.Precision.HIGH
VMEM_LIMIT = 60000 * 1024


def depth_tables(count):
    index = jnp.arange(count, dtype=jnp.float32)
    angle = jnp.pi * index[:, None] * index[None, :] / (count - 1)
    ends = jnp.where((index == 0) | (index == count - 1), 2.0, 1.0)
    forward = jnp.cos(angle)
    backward = 2.0 / (count - 1) * jnp.cos(angle) / (ends[:, None] * ends[None, :])
    return (forward, backward)


def hartley_table(count):
    index = jnp.arange(count, dtype=jnp.int32)
    phase = index[:, None] * index[None, :] % count
    angle = phase.astype(jnp.float32) * (2.0 * math.pi / count)
    return (jnp.cos(angle) + jnp.sin(angle)) / math.sqrt(count)


def wave_square(index, count):
    folded = jnp.minimum(index, count - index).astype(jnp.float32)
    scaled = 2.0 * jnp.pi * folded / count
    return scaled * scaled


def part(axis, size, index):
    if axis == 0:
        return (pl.ds(index * size, size),)
    start = pl.multiple_of(index * size, 128 if axis == 2 else 8)
    return (slice(None),) * axis + (pl.ds(start, size),)


def exchange_kernel(name, count, split, concat, x_ref, o_ref, own_sem, send_sems, recv_sems):
    me = lax.axis_index(name)
    split_size = x_ref.shape[split] // count
    concat_size = x_ref.shape[concat]
    barrier = pltpu.get_barrier_semaphore()
    for step in range(1, count):
        peer = lax.rem(me + step, count)
        pl.semaphore_signal(barrier, inc=1, device_id={name: peer}, device_id_type=MESH)
    pl.semaphore_wait(barrier, count - 1)
    copies = []
    for step in range(1, count):
        peer = lax.rem(me + step, count)
        copy = pltpu.make_async_remote_copy(
            src_ref=x_ref.at[part(split, split_size, peer)],
            dst_ref=o_ref.at[part(concat, concat_size, me)],
            send_sem=send_sems.at[step - 1],
            recv_sem=recv_sems.at[step - 1],
            device_id={name: peer},
            device_id_type=MESH,
        )
        copy.start()
        copies.append(copy)
    own = pltpu.make_async_copy(
        x_ref.at[part(split, split_size, me)], o_ref.at[part(concat, concat_size, me)], own_sem
    )
    own.start()
    own.wait()
    for copy in copies:
        copy.wait()


def exchange(x, name, split, concat, ident):
    count = lax.axis_size(name)
    split_size = x.shape[split] // count
    concat_size = x.shape[concat]
    units = (1, 8, 128)
    if split_size % units[split] or concat_size % units[concat]:
        return lax.all_to_all(x, name, split_axis=split, concat_axis=concat, tiled=True)
    shape = list(x.shape)
    shape[split] = split_size
    shape[concat] = concat_size * count
    return pl.pallas_call(
        functools.partial(exchange_kernel, name, count, split, concat),
        out_shape=jax.ShapeDtypeStruct(tuple(shape), x.dtype),
        in_specs=[pl.BlockSpec(memory_space=pl.ANY)],
        out_specs=pl.BlockSpec(memory_space=pl.ANY),
        scratch_shapes=[
            pltpu.SemaphoreType.DMA,
            pltpu.SemaphoreType.DMA((count - 1,)),
            pltpu.SemaphoreType.DMA((count - 1,)),
        ],
        compiler_params=pltpu.CompilerParams(collective_id=ident, has_side_effects=True),
        name="exchange_" + name + str(ident),
    )(x)


def table_halves(x):
    high = lax.reduce_precision(x, 8, 7)
    return high.astype(jnp.bfloat16), (x - high).astype(jnp.bfloat16)


def halves(x):
    high = x.astype(jnp.bfloat16)
    low = (x - high.astype(jnp.float32)).astype(jnp.bfloat16)
    return high, low


def dot3(a, b, dims=(((1,), (0,)), ((), ()))):
    a_high, a_low = a
    b_high, b_low = b
    dot = functools.partial(lax.dot_general, dimension_numbers=dims, preferred_element_type=jnp.float32)
    return dot(a_high, b_high) + (dot(a_high, b_low) + dot(a_low, b_high))


def lateral_kernel(group, high_ref, low_ref, columns_ref, visc_ref, out_ref):
    table = (high_ref[...], low_ref[...])
    columns = jnp.concatenate([columns_ref[i] for i in range(group)], axis=1)
    physical = dot3(table, halves(columns))
    visc = jnp.concatenate([visc_ref[i].T for i in range(group)], axis=1)
    stress = visc * jnp.exp(jnp.log(1.0 + physical * physical) * (-1.0 / 3.0)) * physical
    back = dot3(table, halves(stress))
    width = back.shape[1] // group
    for i in range(group):
        out_ref[i] = back[:, i * width:(i + 1) * width]


def lateral_stage(table, columns, visc_base):
    depth, total_y, cells_x = columns.shape
    group = 2 if depth % 2 == 0 and cells_x % 128 == 0 else 1
    return pl.pallas_call(
        functools.partial(lateral_kernel, group),
        grid=(depth // group,),
        out_shape=jax.ShapeDtypeStruct(columns.shape, columns.dtype),
        in_specs=[
            pl.BlockSpec((total_y, total_y), lambda z: (0, 0)),
            pl.BlockSpec((total_y, total_y), lambda z: (0, 0)),
            pl.BlockSpec((group, total_y, cells_x), lambda z: (z, 0, 0)),
            pl.BlockSpec((group, cells_x, total_y), lambda z: (z, 0, 0)),
        ],
        out_specs=pl.BlockSpec((group, total_y, cells_x), lambda z: (z, 0, 0)),
        compiler_params=pltpu.CompilerParams(vmem_limit_bytes=VMEM_LIMIT),
        name="lateral_stage",
    )(*table, columns, visc_base)


def lines_kernel(high_ref, low_ref, x_ref, out_ref):
    out_ref[...] = dot3(halves(x_ref[...]), (high_ref[...], low_ref[...]))


def lines_stage(table, x):
    depth, rows, total = x.shape
    flat = x.reshape(depth * rows, total)
    tile = math.gcd(depth * rows, 256)
    out = pl.pallas_call(
        lines_kernel,
        grid=(depth * rows // tile,),
        out_shape=jax.ShapeDtypeStruct(flat.shape, flat.dtype),
        in_specs=[
            pl.BlockSpec((total, total), lambda i: (0, 0)),
            pl.BlockSpec((total, total), lambda i: (0, 0)),
            pl.BlockSpec((tile, total), lambda i: (i, 0)),
        ],
        out_specs=pl.BlockSpec((tile, total), lambda i: (i, 0)),
        compiler_params=pltpu.CompilerParams(vmem_limit_bytes=VMEM_LIMIT),
        name="lines_stage",
    )(*table, flat)
    return out.reshape(x.shape)


def local_plain(mode_field, forcing, visc_base, depth_inverse):
    depth_count = mode_field.shape[0]
    rows_y = mode_field.shape[1]
    cols_x = mode_field.shape[2]
    total_y = rows_y * lax.axis_size("px")
    total_x = cols_x * lax.axis_size("py")
    cell_total = depth_count * total_y * total_x
    forward, backward = depth_tables(depth_count)
    table_x = table_halves(hartley_table(total_x))
    table_y = table_halves(hartley_table(total_y))
    index_y = lax.axis_index("px") * rows_y + jnp.arange(rows_y, dtype=jnp.int32)
    index_x = lax.axis_index("py") * cols_x + jnp.arange(cols_x, dtype=jnp.int32)
    lateral = wave_square(index_y, total_y)[:, None] + wave_square(index_x, total_x)[None, :]
    field = mode_field
    partials = []
    for sweep in range(ITERS):
        points = jnp.einsum("jm,myx->jyx", forward, field, precision=HIGH)
        lines = exchange(points, "py", 0, 2, 0)
        lines = lines_stage(table_x, lines)
        columns = exchange(lines, "px", 2, 1, 1)
        returned = lateral_stage(table_y, columns, visc_base)
        returned = exchange(returned, "px", 1, 2, 2)
        returned = lines_stage(table_x, returned)
        spectral = exchange(returned, "py", 2, 0, 3)
        viscous = jnp.einsum("mj,jyx->myx", backward, spectral, precision=HIGH)
        residual = forcing - (lateral * field + viscous)
        squares = jnp.sum(residual * residual)
        partials.append(squares)
        correction = jnp.einsum("xmn,nyx->myx", depth_inverse, residual, precision=HIGH)
        field = field + correction / (1.0 + lateral)
    norm_values = lax.psum(jnp.stack(partials), ("px", "py")) / cell_total
    return (field, norm_values)


def hartley_factors(count, step):
    line = np.arange(count)
    coarse = 2.0 * np.pi * (np.arange(count // step)[:, None] * step * line[None, :] % count) / count
    fine = 2.0 * np.pi * (np.arange(step)[:, None] * line[None, :] % count) / count
    scale = 1.0 / np.sqrt(count)
    parts = (
        (np.cos(coarse) + np.sin(coarse)) * scale,
        (np.cos(coarse) - np.sin(coarse)) * scale,
        np.cos(fine),
        np.sin(fine),
    )
    return tuple(jnp.asarray(part, jnp.float32) for part in parts)


def depth_factors(count):
    index = np.arange(count)
    angle = np.pi * (index[:, None] * index[None, :] % (2 * (count - 1))) / (count - 1)
    ends = np.where((index == 0) | (index == count - 1), 2.0, 1.0)
    forward = np.cos(angle)
    backward = 2.0 / (count - 1) * np.cos(angle) / (ends[:, None] * ends[None, :])
    return jnp.asarray(np.stack([forward, backward]), jnp.float32)


FINE = 32
SUB = 8


def fused_kernel(
    sizes, field_hbm, forcing_hbm, visc_hbm, inverse_hbm, lateral_ref, scale_ref, depth_ref,
    xp_ref, xm_ref, xc_ref, xs_ref, yp_ref, ym_ref, yc_ref, ys_ref,
    out_hbm, norm_ref,
    field, forcing, visc, inverse, tx_high, tx_low, ty_high, ty_low, kron_high, kron_low,
    send_p, lines, send_f, columns, send_b, returned, send_s, spectral,
    x_high, x_low, resid, correct, norm_sum, norm_send, norm_py, norm_px,
    load_sem, out_sem, p_send, p_recv, f_send, f_recv, b_send, b_recv, s_send, s_recv, n_send, n_recv,
):
    P, Q, Z, RY, W, DL, XB, KC, C, DG, iters, cell_total = sizes
    i = lax.axis_index("px")
    q = lax.axis_index("py")
    groups = DL // DG
    pairs_per_group = DG // 2

    def remote(src, dst, send, recv, name, peer):
        pltpu.make_async_remote_copy(
            src_ref=src, dst_ref=dst, send_sem=send, recv_sem=recv,
            device_id={name: peer}, device_id_type=MESH,
        ).start()

    def local_copy(src, dst, sem):
        pltpu.make_async_copy(src, dst, sem).start()

    def wait_bytes(ref, sem):
        pltpu.make_async_copy(ref, ref, sem).wait()

    loads = [(field_hbm, field), (forcing_hbm, forcing), (visc_hbm, visc), (inverse_hbm, inverse)]
    for slot, (src, dst) in enumerate(loads):
        local_copy(src, dst, load_sem.at[slot])

    barrier = pltpu.get_barrier_semaphore()
    for step in range(1, P):
        pl.semaphore_signal(barrier, inc=1, device_id={"px": lax.rem(i + step, P)}, device_id_type=MESH)
    for step in range(1, Q):
        pl.semaphore_signal(barrier, inc=1, device_id={"py": lax.rem(q + step, Q)}, device_id_type=MESH)
    pl.semaphore_wait(barrier, P + Q - 2)

    ZS = Z * SUB
    row = lax.broadcasted_iota(jnp.int32, (ZS, Z), 0)
    col = lax.broadcasted_iota(jnp.int32, (ZS, Z), 1)
    spread = jnp.where(row // SUB == col, 1.0, 0.0).astype(jnp.bfloat16)
    row_t = lax.broadcasted_iota(jnp.int32, (Z, ZS), 0)
    col_t = lax.broadcasted_iota(jnp.int32, (Z, ZS), 1)
    spread_t = jnp.where(col_t // SUB == row_t, 1.0, 0.0).astype(jnp.bfloat16)
    same = (lax.broadcasted_iota(jnp.int32, (ZS, ZS), 0) % SUB) == (
        lax.broadcasted_iota(jnp.int32, (ZS, ZS), 1) % SUB
    )
    for which in range(2):
        for half, target in zip(halves(depth_ref[which]), (kron_high, kron_low)):
            tall = jnp.dot(spread, half, preferred_element_type=jnp.float32).astype(jnp.bfloat16)
            full = jnp.dot(tall, spread_t, preferred_element_type=jnp.float32)
            target[which] = jnp.where(same, full, 0.0).astype(jnp.bfloat16)

    def make_table(p_ref, m_ref, c_ref, s_ref, store):
        cosine, sine = c_ref, s_ref

        def body(a, carry):
            plus = p_ref[pl.ds(a, 1), :]
            minus = m_ref[pl.ds(a, 1), :]
            high, low = halves(plus * cosine[...] + minus * sine[...])
            store(pl.multiple_of(a * FINE, FINE), high, low)
            return carry

        lax.fori_loop(0, p_ref.shape[0], body, 0)

    def store_x(start, high, low):
        for n in range(Q):
            tx_high[n, pl.ds(start, FINE), :] = high[:, n * W:(n + 1) * W]
            tx_low[n, pl.ds(start, FINE), :] = low[:, n * W:(n + 1) * W]

    def store_y(start, high, low):
        ty_high[pl.ds(start, FINE), :] = high
        ty_low[pl.ds(start, FINE), :] = low

    def kron_dot(which, x):
        return dot3((kron_high[which], kron_low[which]), halves(x.reshape(ZS, W))).reshape(Z, SUB, W)

    def transform(store):
        def body(s, carry):
            n = lax.rem(q + Q // 2 + s, Q)
            store(n, dot3((x_high[...], x_low[...]), (tx_high[n], tx_low[n])))
            return carry

        lax.fori_loop(0, Q, body, 0)

    def split(block, start, width):
        high, low = halves(block.reshape(DL * KC, width))
        x_high[:, start:start + width] = high
        x_low[:, start:start + width] = low

    def back_step(c):
        wait_bytes(returned.at[c], b_recv.at[c])
        wait_bytes(send_f.at[c, pl.ds(0, P - 1)], f_send.at[c])
        for p in range(P):
            split(returned[c, p], p * XB, XB)

        def store(n, value):
            send_s[c, n] = value.reshape(DL, KC, W)

            @pl.when(n != q)
            def _():
                remote(send_s.at[c, n], spectral.at[c, pl.ds(q * DL, DL)], s_send.at[c], s_recv.at[c], "py", n)

            @pl.when(n == q)
            def _():
                local_copy(send_s.at[c, n], spectral.at[c, pl.ds(q * DL, DL)], s_recv.at[c])

        transform(store)

    def solve(c, turn):
        wait_bytes(spectral.at[c], s_recv.at[c])
        wait_bytes(send_s.at[c, pl.ds(0, Q - 1)], s_send.at[c])
        wait_bytes(returned.at[c, pl.ds(0, P - 1)], b_send.at[c])

        def residual(t, carry):
            at = pl.ds(pl.multiple_of(t * SUB, SUB), SUB)
            rows = pl.ds(pl.multiple_of(c * KC + t * SUB, SUB), SUB)
            viscous = kron_dot(1, spectral[c, :, at, :])
            value = forcing[:, rows, :] - (lateral_ref[rows, :][None] * field[:, rows, :] + viscous)
            resid[:, at, :] = value
            norm_sum[turn - 1] += jnp.sum(value * value, axis=0)
            return carry

        lax.fori_loop(0, KC // SUB, residual, 0)

        quads = SUB // 4

        def correction(b, carry):
            t = b // (W // 128)
            lane = pl.multiple_of(lax.rem(b, W // 128) * 128, 128)
            at = pl.ds(pl.multiple_of(t * SUB, SUB), SUB)
            for quad in range(quads):
                def body(n, sums):
                    mix = inverse[n, :, pl.ds(lane, 128)]
                    r = resid[n, at, pl.ds(lane, 128)]
                    return tuple(
                        total + mix * r[quad * 4 + k:quad * 4 + k + 1, :] for k, total in enumerate(sums)
                    )

                zero = jnp.zeros((Z, 128), jnp.float32)
                sums = lax.fori_loop(0, Z, body, (zero,) * 4, unroll=2)
                for k in range(4):
                    correct[t, quad * 4 + k, :, pl.ds(lane, 128)] = sums[k]
            return carry

        lax.fori_loop(0, KC // SUB * (W // 128), correction, 0)

        def update(u, carry):
            t = u // (Z // 8)
            m = pl.ds(pl.multiple_of(lax.rem(u, Z // 8) * 8, 8), 8)
            rows = pl.ds(pl.multiple_of(c * KC + t * SUB, SUB), SUB)
            value = jnp.swapaxes(correct[t, :, m, :], 0, 1)
            field[m, rows, :] += value * scale_ref[rows, :][None]
            return carry

        lax.fori_loop(0, KC // SUB * (Z // 8), update, 0)

    def points(c):
        def body(t, carry):
            at = pl.ds(pl.multiple_of(t * SUB, SUB), SUB)
            rows = pl.ds(pl.multiple_of(c * KC + t * SUB, SUB), SUB)
            send_p[c, :, at, :] = kron_dot(0, field[:, rows, :])
            return carry

        lax.fori_loop(0, KC // SUB, body, 0)
        for step in range(1, Q):
            n = lax.rem(q + (Q // 2 + step - 1 if step <= Q - Q // 2 else step - (Q - Q // 2)), Q)
            remote(send_p.at[c, pl.ds(n * DL, DL)], lines.at[c, q], p_send.at[c], p_recv.at[c], "py", n)
        local_copy(send_p.at[c, pl.ds(q * DL, DL)], lines.at[c, q], p_recv.at[c])

    def line_step(c):
        wait_bytes(lines.at[c], p_recv.at[c])
        wait_bytes(send_p.at[c, pl.ds(0, Z - DL)], p_send.at[c])
        for n in range(Q):
            split(lines[c, n], n * W, W)
        per = W // XB

        def store(n, value):
            for k in range(per):
                send_f[c, n * per + k] = value[:, k * XB:(k + 1) * XB].reshape(DL, KC, XB)

        transform(store)
        mine = pl.ds(pl.multiple_of(i * RY + c * KC, SUB), KC)

        def send(g, carry):
            depths = pl.ds(g * DG, DG)
            for step in range(1, P):
                peer = lax.rem(i + P // 2 + step - 1 if step <= P // 2 else i + step - P // 2, P)
                remote(
                    send_f.at[c, peer, depths], columns.at[depths, mine], f_send.at[c], f_recv.at[g], "px", peer
                )
            local_copy(send_f.at[c, i, depths], columns.at[depths, mine], f_recv.at[g])
            return carry

        lax.fori_loop(0, groups, send, 0)

    def send_back(c, depths):
        for step in range(1, P):
            peer = lax.rem(i + P // 2 + step - 1 if step <= P // 2 else i + step - P // 2, P)
            rows = pl.ds(pl.multiple_of(peer * RY + c * KC, SUB), KC)
            remote(send_b.at[depths, rows], returned.at[c, i, depths], b_send.at[c], b_recv.at[c], "px", peer)
        rows = pl.ds(pl.multiple_of(i * RY + c * KC, SUB), KC)
        local_copy(send_b.at[depths, rows], returned.at[c, i, depths], b_recv.at[c])

    def lateral_step():
        def body(pair, carry):
            g = pair // pairs_per_group

            @pl.when(lax.rem(pair, pairs_per_group) == 0)
            def _():
                wait_bytes(columns.at[pl.ds(g * DG, DG)], f_recv.at[g])

            table = (ty_high[...], ty_low[...])
            block = jnp.concatenate([columns[2 * pair + k] for k in range(2)], axis=1)
            physical = dot3(table, halves(block))
            base = jnp.concatenate([visc[2 * pair + k].T for k in range(2)], axis=1)
            stress = base * jnp.exp(jnp.log(1.0 + physical * physical) * (-1.0 / 3.0)) * physical
            back = dot3(table, halves(stress))
            for k in range(2):
                send_b[2 * pair + k] = back[:, k * XB:(k + 1) * XB]

            @pl.when(lax.rem(pair, pairs_per_group) == pairs_per_group - 1)
            def _():
                send_back(0, pl.ds(g * DG, DG))

            return carry

        lax.fori_loop(0, DL // 2, body, 0)

        def rest(c, carry):
            send_back(c, pl.ds(0, DL))
            return carry

        lax.fori_loop(1, C, rest, 0)

    norm_sum[...] = jnp.zeros_like(norm_sum)
    wait_bytes(field, load_sem.at[0])

    def turn_body(turn, carry):
        def step(t, inner):
            @pl.when((turn > 0) & (t < C))
            def _():
                back_step(t)

            @pl.when((t >= 1) & (t <= C))
            def _():
                c = t - 1

                @pl.when(turn > 0)
                def _():
                    solve(c, turn)

                @pl.when(turn < iters)
                def _():
                    points(c)

                @pl.when(turn == iters)
                def _():
                    rows = pl.ds(pl.multiple_of(c * KC, SUB), KC)
                    local_copy(field.at[:, rows], out_hbm.at[:, rows], out_sem.at[c])

            @pl.when((turn == 0) & (t == 1))
            def _():
                make_table(xp_ref, xm_ref, xc_ref, xs_ref, store_x)
                make_table(yp_ref, ym_ref, yc_ref, ys_ref, store_y)
                wait_bytes(forcing, load_sem.at[1])
                wait_bytes(visc, load_sem.at[2])
                wait_bytes(inverse, load_sem.at[3])

            @pl.when((turn < iters) & (t >= 2))
            def _():
                line_step(t - 2)

            return inner

        lax.fori_loop(0, C + 2, step, 0)

        @pl.when(turn < iters)
        def _():
            lateral_step()

        return carry

    lax.fori_loop(0, iters + 1, turn_body, 0)

    total = norm_sum[...]
    norm_send[0] = sum(total[:, :, k * 128:(k + 1) * 128] for k in range(W // 128))
    for step in range(1, Q):
        remote(norm_send.at[0], norm_py.at[q], n_send.at[0], n_recv.at[0], "py", lax.rem(q + step, Q))
    local_copy(norm_send.at[0], norm_py.at[q], n_recv.at[0])
    wait_bytes(norm_py, n_recv.at[0])
    wait_bytes(norm_py.at[pl.ds(0, Q - 1)], n_send.at[0])
    norm_send[1] = sum(norm_py[k] for k in range(Q))
    for step in range(1, P):
        remote(norm_send.at[1], norm_px.at[i], n_send.at[1], n_recv.at[1], "px", lax.rem(i + step, P))
    local_copy(norm_send.at[1], norm_px.at[i], n_recv.at[1])
    wait_bytes(norm_px, n_recv.at[1])
    wait_bytes(norm_px.at[pl.ds(0, P - 1)], n_send.at[1])
    whole = sum(norm_px[k] for k in range(P))
    whole = jnp.sum(jnp.sum(whole, axis=1), axis=1, keepdims=True)
    norm_ref[...] = jnp.broadcast_to(whole / cell_total, norm_ref.shape)
    for c in range(C):
        rows = pl.ds(c * KC, KC)
        pltpu.make_async_copy(field.at[:, rows], out_hbm.at[:, rows], out_sem.at[c]).wait()


def fused_plan(shape, P, Q):
    Z, RY, W = shape
    NX = W * Q
    if Z % Q or NX % P or P < 2 or Q < 2 or Q % 2 or P % 2:
        return None
    DL, XB = Z // Q, NX // P
    KC = 16
    if RY % KC or XB % 128 or W % XB or DL % 4 or Z % 8 or NX % FINE or (RY * P) % FINE:
        return None
    arrays = 12 * Z * RY * W * 4 + NX * NX * 4 + (RY * P) ** 2 * 4 + (Z * SUB) ** 2 * 8
    arrays += DL * KC * NX * 4 + Z * KC * W * 8
    if arrays > 60 * 2**20:
        return None
    return (P, Q, Z, RY, W, DL, XB, KC, RY // KC, 4, ITERS)


def fused(plan, mode_field, forcing, visc_base, depth_inverse):
    P, Q, Z, RY, W, DL, XB, KC, C, DG, iters = plan
    NX, NY = W * Q, RY * P
    index_y = lax.axis_index("px") * RY + jnp.arange(RY, dtype=jnp.int32)
    index_x = lax.axis_index("py") * W + jnp.arange(W, dtype=jnp.int32)
    lateral = wave_square(index_y, NY)[:, None] + wave_square(index_x, NX)[None, :]
    inverse = jnp.transpose(depth_inverse, (2, 1, 0))
    f32, bf16 = jnp.float32, jnp.bfloat16
    vmem = pl.BlockSpec(memory_space=pltpu.VMEM)
    anywhere = pl.BlockSpec(memory_space=pl.ANY)
    dma = pltpu.SemaphoreType.DMA
    out, norms = pl.pallas_call(
        functools.partial(fused_kernel, plan + (float(Z * NX * NY),)),
        out_shape=(
            jax.ShapeDtypeStruct(mode_field.shape, f32),
            jax.ShapeDtypeStruct((iters, 128), f32),
        ),
        in_specs=[anywhere] * 4 + [vmem] * 11,
        out_specs=(anywhere, vmem),
        scratch_shapes=[
            pltpu.VMEM((Z, RY, W), f32),
            pltpu.VMEM((Z, RY, W), f32),
            pltpu.VMEM((DL, XB, NY), f32),
            pltpu.VMEM((Z, Z, W), f32),
            pltpu.VMEM((Q, NX, W), bf16),
            pltpu.VMEM((Q, NX, W), bf16),
            pltpu.VMEM((NY, NY), bf16),
            pltpu.VMEM((NY, NY), bf16),
            pltpu.VMEM((2, Z * SUB, Z * SUB), bf16),
            pltpu.VMEM((2, Z * SUB, Z * SUB), bf16),
            pltpu.VMEM((C, Z, KC, W), f32),
            pltpu.VMEM((C, Q, DL, KC, W), f32),
            pltpu.VMEM((C, P, DL, KC, XB), f32),
            pltpu.VMEM((DL, NY, XB), f32),
            pltpu.VMEM((DL, NY, XB), f32),
            pltpu.VMEM((C, P, DL, KC, XB), f32),
            pltpu.VMEM((C, Q, DL, KC, W), f32),
            pltpu.VMEM((C, Z, KC, W), f32),
            pltpu.VMEM((DL * KC, NX), bf16),
            pltpu.VMEM((DL * KC, NX), bf16),
            pltpu.VMEM((Z, KC, W), f32),
            pltpu.VMEM((KC // SUB, SUB, Z, W), f32),
            pltpu.VMEM((iters, SUB, W), f32),
            pltpu.VMEM((2, iters, SUB, 128), f32),
            pltpu.VMEM((Q, iters, SUB, 128), f32),
            pltpu.VMEM((P, iters, SUB, 128), f32),
            dma((4,)),
            dma((C,)),
            dma((C,)), dma((C,)),
            dma((C,)), dma((DL // DG,)),
            dma((C,)), dma((C,)),
            dma((C,)), dma((C,)),
            dma((2,)), dma((2,)),
        ],
        compiler_params=pltpu.CompilerParams(
            collective_id=7, has_side_effects=True, vmem_limit_bytes=67043328
        ),
        name="fused",
    )(
        mode_field, forcing, visc_base, inverse, lateral, 1.0 / (1.0 + lateral), depth_factors(Z),
        *hartley_factors(NX, FINE), *hartley_factors(NY, FINE),
    )
    return out, norms[:, 0]


def local(mode_field, forcing, visc_base, depth_inverse):
    plan = fused_plan(mode_field.shape, lax.axis_size("px"), lax.axis_size("py"))
    if plan is None:
        return local_plain(mode_field, forcing, visc_base, depth_inverse)
    return fused(plan, mode_field, forcing, visc_base, depth_inverse)


def solution(mesh):
    placed = (P(None, "px", "py"), P(None, "px", "py"), P("py", "px", None), P("py", None, None))
    return jax.shard_map(
        local, mesh=mesh, in_specs=placed, out_specs=(P(None, "px", "py"), P()), check_vma=False
    )
```

```python
import functools
import math

import jax
import jax.numpy as jnp
import numpy as np
from jax import lax
from jax.experimental import pallas as pl
from jax.experimental.pallas import tpu as pltpu
from jax.sharding import PartitionSpec as P

ITERS = 2
MESH = pl.DeviceIdType.MESH
HIGH = lax.Precision.HIGH
VMEM_LIMIT = 60000 * 1024


def depth_tables(count):
    index = jnp.arange(count, dtype=jnp.float32)
    angle = jnp.pi * index[:, None] * index[None, :] / (count - 1)
    ends = jnp.where((index == 0) | (index == count - 1), 2.0, 1.0)
    forward = jnp.cos(angle)
    backward = 2.0 / (count - 1) * jnp.cos(angle) / (ends[:, None] * ends[None, :])
    return (forward, backward)


def hartley_table(count):
    index = jnp.arange(count, dtype=jnp.int32)
    phase = index[:, None] * index[None, :] % count
    angle = phase.astype(jnp.float32) * (2.0 * math.pi / count)
    return (jnp.cos(angle) + jnp.sin(angle)) / math.sqrt(count)


def wave_square(index, count):
    folded = jnp.minimum(index, count - index).astype(jnp.float32)
    scaled = 2.0 * jnp.pi * folded / count
    return scaled * scaled


def part(axis, size, index):
    if axis == 0:
        return (pl.ds(index * size, size),)
    start = pl.multiple_of(index * size, 128 if axis == 2 else 8)
    return (slice(None),) * axis + (pl.ds(start, size),)


def exchange_kernel(name, count, split, concat, x_ref, o_ref, own_sem, send_sems, recv_sems):
    me = lax.axis_index(name)
    split_size = x_ref.shape[split] // count
    concat_size = x_ref.shape[concat]
    barrier = pltpu.get_barrier_semaphore()
    for step in range(1, count):
        peer = lax.rem(me + step, count)
        pl.semaphore_signal(barrier, inc=1, device_id={name: peer}, device_id_type=MESH)
    pl.semaphore_wait(barrier, count - 1)
    copies = []
    for step in range(1, count):
        peer = lax.rem(me + step, count)
        copy = pltpu.make_async_remote_copy(
            src_ref=x_ref.at[part(split, split_size, peer)],
            dst_ref=o_ref.at[part(concat, concat_size, me)],
            send_sem=send_sems.at[step - 1],
            recv_sem=recv_sems.at[step - 1],
            device_id={name: peer},
            device_id_type=MESH,
        )
        copy.start()
        copies.append(copy)
    own = pltpu.make_async_copy(
        x_ref.at[part(split, split_size, me)], o_ref.at[part(concat, concat_size, me)], own_sem
    )
    own.start()
    own.wait()
    for copy in copies:
        copy.wait()


def exchange(x, name, split, concat, ident):
    count = lax.axis_size(name)
    split_size = x.shape[split] // count
    concat_size = x.shape[concat]
    units = (1, 8, 128)
    if split_size % units[split] or concat_size % units[concat]:
        return lax.all_to_all(x, name, split_axis=split, concat_axis=concat, tiled=True)
    shape = list(x.shape)
    shape[split] = split_size
    shape[concat] = concat_size * count
    return pl.pallas_call(
        functools.partial(exchange_kernel, name, count, split, concat),
        out_shape=jax.ShapeDtypeStruct(tuple(shape), x.dtype),
        in_specs=[pl.BlockSpec(memory_space=pl.ANY)],
        out_specs=pl.BlockSpec(memory_space=pl.ANY),
        scratch_shapes=[
            pltpu.SemaphoreType.DMA,
            pltpu.SemaphoreType.DMA((count - 1,)),
            pltpu.SemaphoreType.DMA((count - 1,)),
        ],
        compiler_params=pltpu.CompilerParams(collective_id=ident, has_side_effects=True),
        name="exchange_" + name + str(ident),
    )(x)


def table_halves(x):
    high = lax.reduce_precision(x, 8, 7)
    return high.astype(jnp.bfloat16), (x - high).astype(jnp.bfloat16)


def halves(x):
    high = x.astype(jnp.bfloat16)
    low = (x - high.astype(jnp.float32)).astype(jnp.bfloat16)
    return high, low


def dot3(a, b, dims=(((1,), (0,)), ((), ()))):
    a_high, a_low = a
    b_high, b_low = b
    dot = functools.partial(lax.dot_general, dimension_numbers=dims, preferred_element_type=jnp.float32)
    return dot(a_high, b_high) + (dot(a_high, b_low) + dot(a_low, b_high))


def lateral_kernel(group, high_ref, low_ref, columns_ref, visc_ref, out_ref):
    table = (high_ref[...], low_ref[...])
    columns = jnp.concatenate([columns_ref[i] for i in range(group)], axis=1)
    physical = dot3(table, halves(columns))
    visc = jnp.concatenate([visc_ref[i].T for i in range(group)], axis=1)
    stress = visc * jnp.exp(jnp.log(1.0 + physical * physical) * (-1.0 / 3.0)) * physical
    back = dot3(table, halves(stress))
    width = back.shape[1] // group
    for i in range(group):
        out_ref[i] = back[:, i * width:(i + 1) * width]


def lateral_stage(table, columns, visc_base):
    depth, total_y, cells_x = columns.shape
    group = 2 if depth % 2 == 0 and cells_x % 128 == 0 else 1
    return pl.pallas_call(
        functools.partial(lateral_kernel, group),
        grid=(depth // group,),
        out_shape=jax.ShapeDtypeStruct(columns.shape, columns.dtype),
        in_specs=[
            pl.BlockSpec((total_y, total_y), lambda z: (0, 0)),
            pl.BlockSpec((total_y, total_y), lambda z: (0, 0)),
            pl.BlockSpec((group, total_y, cells_x), lambda z: (z, 0, 0)),
            pl.BlockSpec((group, cells_x, total_y), lambda z: (z, 0, 0)),
        ],
        out_specs=pl.BlockSpec((group, total_y, cells_x), lambda z: (z, 0, 0)),
        compiler_params=pltpu.CompilerParams(vmem_limit_bytes=VMEM_LIMIT),
        name="lateral_stage",
    )(*table, columns, visc_base)


def lines_kernel(high_ref, low_ref, x_ref, out_ref):
    out_ref[...] = dot3(halves(x_ref[...]), (high_ref[...], low_ref[...]))


def lines_stage(table, x):
    depth, rows, total = x.shape
    flat = x.reshape(depth * rows, total)
    tile = math.gcd(depth * rows, 256)
    out = pl.pallas_call(
        lines_kernel,
        grid=(depth * rows // tile,),
        out_shape=jax.ShapeDtypeStruct(flat.shape, flat.dtype),
        in_specs=[
            pl.BlockSpec((total, total), lambda i: (0, 0)),
            pl.BlockSpec((total, total), lambda i: (0, 0)),
            pl.BlockSpec((tile, total), lambda i: (i, 0)),
        ],
        out_specs=pl.BlockSpec((tile, total), lambda i: (i, 0)),
        compiler_params=pltpu.CompilerParams(vmem_limit_bytes=VMEM_LIMIT),
        name="lines_stage",
    )(*table, flat)
    return out.reshape(x.shape)


def local_plain(mode_field, forcing, visc_base, depth_inverse):
    depth_count = mode_field.shape[0]
    rows_y = mode_field.shape[1]
    cols_x = mode_field.shape[2]
    total_y = rows_y * lax.axis_size("px")
    total_x = cols_x * lax.axis_size("py")
    cell_total = depth_count * total_y * total_x
    forward, backward = depth_tables(depth_count)
    table_x = table_halves(hartley_table(total_x))
    table_y = table_halves(hartley_table(total_y))
    index_y = lax.axis_index("px") * rows_y + jnp.arange(rows_y, dtype=jnp.int32)
    index_x = lax.axis_index("py") * cols_x + jnp.arange(cols_x, dtype=jnp.int32)
    lateral = wave_square(index_y, total_y)[:, None] + wave_square(index_x, total_x)[None, :]
    field = mode_field
    partials = []
    for sweep in range(ITERS):
        points = jnp.einsum("jm,myx->jyx", forward, field, precision=HIGH)
        lines = exchange(points, "py", 0, 2, 0)
        lines = lines_stage(table_x, lines)
        columns = exchange(lines, "px", 2, 1, 1)
        returned = lateral_stage(table_y, columns, visc_base)
        returned = exchange(returned, "px", 1, 2, 2)
        returned = lines_stage(table_x, returned)
        spectral = exchange(returned, "py", 2, 0, 3)
        viscous = jnp.einsum("mj,jyx->myx", backward, spectral, precision=HIGH)
        residual = forcing - (lateral * field + viscous)
        squares = jnp.sum(residual * residual)
        partials.append(squares)
        correction = jnp.einsum("xmn,nyx->myx", depth_inverse, residual, precision=HIGH)
        field = field + correction / (1.0 + lateral)
    norm_values = lax.psum(jnp.stack(partials), ("px", "py")) / cell_total
    return (field, norm_values)


def hartley_factors(count, step):
    line = np.arange(count)
    coarse = 2.0 * np.pi * (np.arange(count // step)[:, None] * step * line[None, :] % count) / count
    fine = 2.0 * np.pi * (np.arange(step)[:, None] * line[None, :] % count) / count
    scale = 1.0 / np.sqrt(count)
    parts = (
        (np.cos(coarse) + np.sin(coarse)) * scale,
        (np.cos(coarse) - np.sin(coarse)) * scale,
        np.cos(fine),
        np.sin(fine),
    )
    return tuple(jnp.asarray(part, jnp.float32) for part in parts)


def depth_factors(count):
    index = np.arange(count)
    angle = np.pi * (index[:, None] * index[None, :] % (2 * (count - 1))) / (count - 1)
    ends = np.where((index == 0) | (index == count - 1), 2.0, 1.0)
    forward = np.cos(angle)
    backward = 2.0 / (count - 1) * np.cos(angle) / (ends[:, None] * ends[None, :])
    spread = np.stack([np.kron(table, np.eye(SUB)) for table in (forward, backward)]).astype(np.float32)
    high = spread.astype(jnp.bfloat16)
    low = (spread - high.astype(np.float32)).astype(jnp.bfloat16)
    return jnp.asarray(high), jnp.asarray(low)


FINE = 32
SUB = 8


def fused_kernel(
    sizes, field_hbm, forcing_hbm, visc_hbm, inverse_hbm, kron_high_hbm, kron_low_hbm, *rest,
):
    factors_hbm, (field, norm_ref), scratch = rest[:8], rest[8:10], rest[10:]
    (
        forcing, visc, inverse, tx_high, tx_low, ty_high, ty_low, kron_high, kron_low,
        send_p, lines, send_f, columns, send_b, returned, send_s, spectral,
        x_both, resid, correct, norm_sum, norm_send, norm_py, norm_px,
        stage, load_sem, stage_sem, field_sem, kron_sem, factor_sem, p_send, p_recv, p_first, f_send, f_recv, b_send, b_recv, b_last, s_send, s_recv, n_send, n_recv,
        lateral_ref, scale_ref, *factors,
    ) = scratch
    P, Q, Z, RY, W, DL, XB, KC, C, DG, iters, cell_total = sizes
    i = lax.axis_index("px")
    q = lax.axis_index("py")
    groups = DL // DG
    early = min(C - 1, max(1, 16 // KC))
    pairs_per_group = DG // 2

    def remote(src, dst, send, recv, name, peer):
        pltpu.make_async_remote_copy(
            src_ref=src, dst_ref=dst, send_sem=send, recv_sem=recv,
            device_id={name: peer}, device_id_type=MESH,
        ).start()

    def local_copy(src, dst, sem):
        pltpu.make_async_copy(src, dst, sem).start()

    def wait_bytes(ref, sem):
        pltpu.make_async_copy(ref, ref, sem).wait()

    for c in range(C):
        rows = pl.ds(c * KC, KC)
        local_copy(field_hbm.at[:, rows], field.at[:, rows], field_sem.at[c])
        if c < 2:
            local_copy(kron_high_hbm.at[c], kron_high.at[c], kron_sem.at[2 * c])
            local_copy(kron_low_hbm.at[c], kron_low.at[c], kron_sem.at[2 * c + 1])

    for slot, (src, dst) in enumerate(zip(factors_hbm, factors)):
        local_copy(src, dst, factor_sem.at[slot])

    barrier = pltpu.get_barrier_semaphore()
    for step in range(1, P):
        pl.semaphore_signal(barrier, inc=1, device_id={"px": lax.rem(i + step, P)}, device_id_type=MESH)
    for step in range(1, Q):
        pl.semaphore_signal(barrier, inc=1, device_id={"py": lax.rem(q + step, Q)}, device_id_type=MESH)
    def make_table(p_ref, m_ref, c_ref, s_ref, store):
        cosine, sine = c_ref, s_ref

        def body(a, carry):
            plus = p_ref[pl.ds(a, 1), :]
            minus = m_ref[pl.ds(a, 1), :]
            high, low = halves(plus * cosine[...] + minus * sine[...])
            store(pl.multiple_of(a * FINE, FINE), high, low)
            return carry

        lax.fori_loop(0, p_ref.shape[0], body, 0)

    def store_x(start, high, low):
        for n in range(Q):
            tx_high[n, pl.ds(start, FINE), :] = high[:, n * W:(n + 1) * W]
            tx_low[n, pl.ds(start, FINE), :] = low[:, n * W:(n + 1) * W]

    def store_y(start, high, low):
        ty_high[pl.ds(start, FINE), :] = high
        ty_low[pl.ds(start, FINE), :] = low

    def kron_dot(which, x):
        return dot3((kron_high[which], kron_low[which]), halves(x.reshape(Z * SUB, W))).reshape(Z, SUB, W)

    def transform(count, store):
        def body(s, carry):
            n = lax.rem(q + Q // 2 + s, Q)
            both = jnp.dot(x_both[:2 * count], tx_high[n], preferred_element_type=jnp.float32)
            cross = jnp.dot(x_both[:count], tx_low[n], preferred_element_type=jnp.float32)
            store(n, both[:count] + (cross + both[count:]))
            return carry

        lax.fori_loop(0, Q, body, 0)

    def split(block, start, width):
        count = block.shape[0] * KC
        high, low = halves(block.reshape(count, width))
        x_both[:count, start:start + width] = high
        x_both[count:2 * count, start:start + width] = low

    def back_part(c, start, count):
        depths = pl.ds(start, count)
        for p in range(P):
            split(returned[c, p, depths], p * XB, XB)

        def store(n, value):
            send_s[c, n, depths] = value.reshape(count, KC, W)
            target = spectral.at[c, pl.ds(q * DL + start, count)]

            @pl.when(n != q)
            def _():
                remote(send_s.at[c, n, depths], target, s_send.at[c], s_recv.at[c], "py", n)

            @pl.when(n == q)
            def _():
                local_copy(send_s.at[c, n, depths], target, s_recv.at[c])

        transform(count * KC, store)

    def back_step(c):
        @pl.when(c < C - 1)
        def _():
            wait_bytes(returned.at[c], b_recv.at[c])
            back_part(c, 0, DL)

        @pl.when(c == C - 1)
        def _():
            def part(g, carry):
                wait_bytes(returned.at[c, :, pl.ds(g * DG, DG)], b_last.at[g])
                back_part(c, g * DG, DG)
                return carry

            lax.fori_loop(0, groups, part, 0)

        wait_bytes(send_f.at[c, pl.ds(0, P - 1)], f_send.at[c])

    def solve(c, turn):
        wait_bytes(spectral.at[c], s_recv.at[c])
        wait_bytes(send_s.at[c, pl.ds(0, Q - 1)], s_send.at[c])
        wait_bytes(returned.at[c, pl.ds(0, P - 1)], b_send.at[c])

        def residual(t, carry):
            at = pl.ds(pl.multiple_of(t * SUB, SUB), SUB)
            rows = pl.ds(pl.multiple_of(c * KC + t * SUB, SUB), SUB)
            viscous = kron_dot(1, spectral[c, :, at, :])
            value = forcing[:, rows, :] - (lateral_ref[rows, :][None] * field[:, rows, :] + viscous)
            resid[:, at, :] = value
            norm_sum[turn - 1] += jnp.sum(value * value, axis=0)
            return carry

        lax.fori_loop(0, KC // SUB, residual, 0)

        last = (turn == iters) & (c == C - 1)

        @pl.when(last)
        def _():
            total = norm_sum[...]
            norm_send[0] = sum(total[:, :, k * 128:(k + 1) * 128] for k in range(W // 128))
            for step in range(1, Q):
                remote(norm_send.at[0], norm_py.at[q], n_send.at[0], n_recv.at[0], "py", lax.rem(q + step, Q))
            local_copy(norm_send.at[0], norm_py.at[q], n_recv.at[0])

        quads = SUB // 4

        def correction(b, carry):
            t = b // (W // 128)
            lane = pl.multiple_of(lax.rem(b, W // 128) * 128, 128)
            at = pl.ds(pl.multiple_of(t * SUB, SUB), SUB)
            for quad in range(quads):
                def body(n, sums):
                    mix = inverse[n, :, pl.ds(lane, 128)]
                    r = resid[n, at, pl.ds(lane, 128)]
                    return tuple(
                        total + mix * r[quad * 4 + k:quad * 4 + k + 1, :] for k, total in enumerate(sums)
                    )

                zero = jnp.zeros((Z, 128), jnp.float32)
                sums = lax.fori_loop(0, Z, body, (zero,) * 4, unroll=2)
                for k in range(4):
                    correct[t, quad * 4 + k, :, pl.ds(lane, 128)] = sums[k]
            return carry

        lax.fori_loop(0, KC // SUB * (W // 128), correction, 0)

        @pl.when(last)
        def _():
            wait_bytes(norm_py, n_recv.at[0])
            wait_bytes(norm_py.at[pl.ds(0, Q - 1)], n_send.at[0])
            norm_send[1] = sum(norm_py[k] for k in range(Q))
            for step in range(1, P):
                remote(norm_send.at[1], norm_px.at[i], n_send.at[1], n_recv.at[1], "px", lax.rem(i + step, P))
            local_copy(norm_send.at[1], norm_px.at[i], n_recv.at[1])

        def update(u, carry):
            t = u // (Z // 8)
            m = pl.ds(pl.multiple_of(lax.rem(u, Z // 8) * 8, 8), 8)
            rows = pl.ds(pl.multiple_of(c * KC + t * SUB, SUB), SUB)
            value = jnp.swapaxes(correct[t, :, m, :], 0, 1)
            field[m, rows, :] += value * scale_ref[rows, :][None]
            return carry

        lax.fori_loop(0, KC // SUB * (Z // 8), update, 0)

    def points(c):
        def body(t, carry):
            at = pl.ds(pl.multiple_of(t * SUB, SUB), SUB)
            rows = pl.ds(pl.multiple_of(c * KC + t * SUB, SUB), SUB)
            send_p[c, :, at, :] = kron_dot(0, field[:, rows, :])
            return carry

        lax.fori_loop(0, KC // SUB, body, 0)

        def ship(start, count, recv):
            for step in range(1, Q):
                n = lax.rem(q + (Q // 2 + step - 1 if step <= Q - Q // 2 else step - (Q - Q // 2)), Q)
                part = send_p.at[c, pl.ds(n * DL + start, count)]
                remote(part, lines.at[c, q, pl.ds(start, count)], p_send.at[c], recv, "py", n)
            part = send_p.at[c, pl.ds(q * DL + start, count)]
            local_copy(part, lines.at[c, q, pl.ds(start, count)], recv)

        @pl.when(c > 0)
        def _():
            ship(0, DL, p_recv.at[c])

        @pl.when(c == 0)
        def _():
            def part(g, carry):
                ship(g * DG, DG, p_first.at[g])
                return carry

            lax.fori_loop(0, groups, part, 0)

    def line_part(c, start, count):
        depths = pl.ds(start, count)
        for n in range(Q):
            split(lines[c, n, depths], n * W, W)
        per = W // XB

        def store(n, value):
            for k in range(per):
                send_f[c, n * per + k, depths] = value[:, k * XB:(k + 1) * XB].reshape(count, KC, XB)

        transform(count * KC, store)

    def line_send(c, g):
        depths = pl.ds(g * DG, DG)
        mine = pl.ds(pl.multiple_of(i * RY + c * KC, SUB), KC)
        for step in range(1, P):
            peer = lax.rem(i + P // 2 + step - 1 if step <= P // 2 else i + step - P // 2, P)
            remote(send_f.at[c, peer, depths], columns.at[depths, mine], f_send.at[c], f_recv.at[g], "px", peer)
        local_copy(send_f.at[c, i, depths], columns.at[depths, mine], f_recv.at[g])

    def line_step(c):
        @pl.when(c > 0)
        def _():
            wait_bytes(lines.at[c], p_recv.at[c])
            line_part(c, 0, DL)

            def send(g, carry):
                line_send(c, g)
                return carry

            lax.fori_loop(0, groups, send, 0)

        @pl.when(c == 0)
        def _():
            def part(g, carry):
                wait_bytes(lines.at[c, :, pl.ds(g * DG, DG)], p_first.at[g])
                line_part(c, g * DG, DG)
                line_send(c, g)
                return carry

            lax.fori_loop(0, groups, part, 0)

        wait_bytes(send_p.at[c, pl.ds(0, Z - DL)], p_send.at[c])

    def send_back(c, depths, recv):
        for step in range(1, P):
            peer = lax.rem(i + P // 2 + step - 1 if step <= P // 2 else i + step - P // 2, P)
            rows = pl.ds(pl.multiple_of(peer * RY + c * KC, SUB), KC)
            remote(send_b.at[depths, rows], returned.at[c, i, depths], b_send.at[c], recv, "px", peer)
        rows = pl.ds(pl.multiple_of(i * RY + c * KC, SUB), KC)
        local_copy(send_b.at[depths, rows], returned.at[c, i, depths], recv)

    def lateral_step():
        def body(pair, carry):
            g = pair // pairs_per_group

            @pl.when(lax.rem(pair, pairs_per_group) == 0)
            def _():
                wait_bytes(columns.at[pl.ds(g * DG, DG)], f_recv.at[g])

            table = (ty_high[...], ty_low[...])
            block = jnp.concatenate([columns[2 * pair + k] for k in range(2)], axis=1)
            physical = dot3(table, halves(block))
            base = jnp.concatenate([visc[2 * pair + k].T for k in range(2)], axis=1)
            stress = base * jnp.exp(jnp.log(1.0 + physical * physical) * (-1.0 / 3.0)) * physical
            back = dot3(table, halves(stress))
            for k in range(2):
                send_b[2 * pair + k] = back[:, k * XB:(k + 1) * XB]

            @pl.when(lax.rem(pair, pairs_per_group) == pairs_per_group - 1)
            def _():
                for c in range(early):
                    send_back(c, pl.ds(g * DG, DG), b_recv.at[c])

            return carry

        lax.fori_loop(0, DL // 2, body, 0)

        def rest(c, carry):
            send_back(c, pl.ds(0, DL), b_recv.at[c])
            return carry

        lax.fori_loop(early, C - 1, rest, 0)

        def final(g, carry):
            send_back(C - 1, pl.ds(g * DG, DG), b_last.at[g])
            return carry

        lax.fori_loop(0, groups, final, 0)

    def make_lateral():
        y = wave_square(i * RY + lax.broadcasted_iota(jnp.int32, (RY, W), 0), RY * P)
        x = wave_square(q * W + lax.broadcasted_iota(jnp.int32, (RY, W), 1), W * Q)
        lateral_ref[...] = y + x
        scale_ref[...] = 1.0 / (1.0 + (y + x))

    def swap_inverse():
        def fetch(b, slot):
            block = pl.ds(pl.multiple_of(b * SUB, SUB), SUB)
            local_copy(inverse_hbm.at[block], stage.at[slot], stage_sem.at[slot])

        fetch(0, 0)

        def body(b, carry):
            slot = lax.rem(b, 2)
            wait_bytes(stage.at[slot], stage_sem.at[slot])

            @pl.when(b + 1 < Z // SUB)
            def _():
                fetch(b + 1, 1 - slot)

            m = pl.ds(pl.multiple_of(b * SUB, SUB), SUB)

            def swap(u, inner):
                n = pl.ds(pl.multiple_of(u * SUB, SUB), SUB)
                inverse[n, m, :] = jnp.swapaxes(stage[slot, :, n, :], 0, 1)
                return inner

            return lax.fori_loop(0, Z // SUB, swap, carry)

        lax.fori_loop(0, Z // SUB, body, 0)

    norm_sum[...] = jnp.zeros_like(norm_sum)
    wait_bytes(kron_high.at[0], kron_sem.at[0])
    wait_bytes(kron_low.at[0], kron_sem.at[1])
    pl.semaphore_wait(barrier, P + Q - 2)

    def turn_body(turn, carry):
        def step(t, inner):
            @pl.when((turn > 0) & (t < C))
            def _():
                back_step(t)

            @pl.when((t >= 1) & (t <= C))
            def _():
                c = t - 1

                @pl.when(turn > 0)
                def _():
                    solve(c, turn)

                @pl.when(turn == 0)
                def _():
                    rows = pl.ds(pl.multiple_of(c * KC, SUB), KC)
                    wait_bytes(field.at[:, rows], field_sem.at[c])

                @pl.when(turn < iters)
                def _():
                    points(c)

            @pl.when((turn == 0) & (t == 1))
            def _():
                for slot, (src, dst) in enumerate(zip(factors_hbm, factors)):
                    wait_bytes(dst, factor_sem.at[slot])
                make_table(*factors[:4], store_x)
                local_copy(forcing_hbm, forcing, load_sem.at[0])
                local_copy(visc_hbm, visc, load_sem.at[1])

            @pl.when((turn < iters) & (t >= 2))
            def _():
                line_step(t - 2)

            @pl.when((turn == 0) & (t == 3))
            def _():
                make_table(*factors[4:], store_y)
                wait_bytes(kron_high.at[1], kron_sem.at[2])
                wait_bytes(kron_low.at[1], kron_sem.at[3])
                make_lateral()
                swap_inverse()
                wait_bytes(forcing, load_sem.at[0])
                wait_bytes(visc, load_sem.at[1])

            return inner

        lax.fori_loop(0, C + 2, step, 0)

        @pl.when(turn < iters)
        def _():
            lateral_step()

        return carry

    lax.fori_loop(0, iters + 1, turn_body, 0)

    wait_bytes(norm_px, n_recv.at[1])
    wait_bytes(norm_px.at[pl.ds(0, P - 1)], n_send.at[1])
    whole = sum(norm_px[k] for k in range(P))
    for k in range(iters):
        norm_ref[k] = jnp.sum(whole[k]) / cell_total


def fused_plan(shape, P, Q):
    Z, RY, W = shape
    NX = W * Q
    if Z % Q or NX % P or P < 2 or Q < 2 or Q % 2 or P % 2:
        return None
    DL, XB = Z // Q, NX // P
    KC = 8
    if RY % KC or XB % 128 or W % XB or DL % 4 or Z % 8 or NX % FINE or (RY * P) % FINE:
        return None
    arrays = 12 * Z * RY * W * 4 + NX * NX * 4 + (RY * P) ** 2 * 4 + (Z * SUB) ** 2 * 8
    arrays += DL * KC * NX * 4 + Z * KC * W * 8
    if arrays > 60 * 2**20:
        return None
    return (P, Q, Z, RY, W, DL, XB, KC, RY // KC, 4, ITERS)


def fused(plan, mode_field, forcing, visc_base, depth_inverse):
    P, Q, Z, RY, W, DL, XB, KC, C, DG, iters = plan
    NX, NY = W * Q, RY * P
    factors = hartley_factors(NX, FINE) + hartley_factors(NY, FINE)
    inverse = jnp.transpose(depth_inverse, (1, 2, 0))
    f32, bf16 = jnp.float32, jnp.bfloat16
    vmem = pl.BlockSpec(memory_space=pltpu.VMEM)
    anywhere = pl.BlockSpec(memory_space=pl.ANY)
    dma = pltpu.SemaphoreType.DMA
    out, norms = pl.pallas_call(
        functools.partial(fused_kernel, plan + (float(Z * NX * NY),)),
        out_shape=(
            pltpu.VMEM(mode_field.shape, f32),
            jax.ShapeDtypeStruct((iters,), f32),
        ),
        in_specs=[anywhere] * 14,
        out_specs=(vmem, pl.BlockSpec(memory_space=pltpu.SMEM)),
        scratch_shapes=[
            pltpu.VMEM((Z, RY, W), f32),
            pltpu.VMEM((DL, XB, NY), f32),
            pltpu.VMEM((Z, Z, W), f32),
            pltpu.VMEM((Q, NX, W), bf16),
            pltpu.VMEM((Q, NX, W), bf16),
            pltpu.VMEM((NY, NY), bf16),
            pltpu.VMEM((NY, NY), bf16),
            pltpu.VMEM((2, Z * SUB, Z * SUB), bf16),
            pltpu.VMEM((2, Z * SUB, Z * SUB), bf16),
            pltpu.VMEM((C, Z, KC, W), f32),
            pltpu.VMEM((C, Q, DL, KC, W), f32),
            pltpu.VMEM((C, P, DL, KC, XB), f32),
            pltpu.VMEM((DL, NY, XB), f32),
            pltpu.VMEM((DL, NY, XB), f32),
            pltpu.VMEM((C, P, DL, KC, XB), f32),
            pltpu.VMEM((C, Q, DL, KC, W), f32),
            pltpu.VMEM((C, Z, KC, W), f32),
            pltpu.VMEM((2 * DL * KC, NX), bf16),
            pltpu.VMEM((Z, KC, W), f32),
            pltpu.VMEM((KC // SUB, SUB, Z, W), f32),
            pltpu.VMEM((iters, SUB, W), f32),
            pltpu.VMEM((2, iters, SUB, 128), f32),
            pltpu.VMEM((Q, iters, SUB, 128), f32),
            pltpu.VMEM((P, iters, SUB, 128), f32),
            pltpu.VMEM((2, SUB, Z, W), f32),
            dma((2,)), dma((2,)), dma((C,)), dma((4,)), dma((8,)),
            dma((C,)), dma((C,)), dma((DL // DG,)),
            dma((C,)), dma((DL // DG,)),
            dma((C,)), dma((C,)), dma((DL // DG,)),
            dma((C,)), dma((C,)),
            dma((2,)), dma((2,)),
            pltpu.VMEM((RY, W), f32),
            pltpu.VMEM((RY, W), f32),
            *(pltpu.VMEM(factor.shape, f32) for factor in factors),
        ],
        compiler_params=pltpu.CompilerParams(
            collective_id=7, has_side_effects=True, vmem_limit_bytes=59 * 1024 * 1024
        ),
        name="fused",
    )(
        mode_field, forcing, visc_base, inverse, *depth_factors(Z), *factors,
    )
    return out, norms


def local(mode_field, forcing, visc_base, depth_inverse):
    plan = fused_plan(mode_field.shape, lax.axis_size("px"), lax.axis_size("py"))
    if plan is None:
        return local_plain(mode_field, forcing, visc_base, depth_inverse)
    return fused(plan, mode_field, forcing, visc_base, depth_inverse)


def solution(mesh):
    placed = (P(None, "px", "py"), P(None, "px", "py"), P("py", "px", None), P("py", None, None))
    return jax.shard_map(
        local, mesh=mesh, in_specs=placed, out_specs=(P(None, "px", "py"), P()), check_vma=False
    )
```

```python
import functools
import math

import jax
import jax.numpy as jnp
import numpy as np
from jax import lax
from jax.experimental import pallas as pl
from jax.experimental.pallas import tpu as pltpu
from jax.sharding import PartitionSpec as P

ITERS = 2
MESH = pl.DeviceIdType.MESH
HIGH = lax.Precision.HIGH
VMEM_LIMIT = 60000 * 1024


def depth_tables(count):
    index = jnp.arange(count, dtype=jnp.float32)
    angle = jnp.pi * index[:, None] * index[None, :] / (count - 1)
    ends = jnp.where((index == 0) | (index == count - 1), 2.0, 1.0)
    forward = jnp.cos(angle)
    backward = 2.0 / (count - 1) * jnp.cos(angle) / (ends[:, None] * ends[None, :])
    return (forward, backward)


def hartley_table(count):
    index = jnp.arange(count, dtype=jnp.int32)
    phase = index[:, None] * index[None, :] % count
    angle = phase.astype(jnp.float32) * (2.0 * math.pi / count)
    return (jnp.cos(angle) + jnp.sin(angle)) / math.sqrt(count)


def wave_square(index, count):
    folded = jnp.minimum(index, count - index).astype(jnp.float32)
    scaled = 2.0 * jnp.pi * folded / count
    return scaled * scaled


def part(axis, size, index):
    if axis == 0:
        return (pl.ds(index * size, size),)
    start = pl.multiple_of(index * size, 128 if axis == 2 else 8)
    return (slice(None),) * axis + (pl.ds(start, size),)


def exchange_kernel(name, count, split, concat, x_ref, o_ref, own_sem, send_sems, recv_sems):
    me = lax.axis_index(name)
    split_size = x_ref.shape[split] // count
    concat_size = x_ref.shape[concat]
    barrier = pltpu.get_barrier_semaphore()
    for step in range(1, count):
        peer = lax.rem(me + step, count)
        pl.semaphore_signal(barrier, inc=1, device_id={name: peer}, device_id_type=MESH)
    pl.semaphore_wait(barrier, count - 1)
    copies = []
    for step in range(1, count):
        peer = lax.rem(me + step, count)
        copy = pltpu.make_async_remote_copy(
            src_ref=x_ref.at[part(split, split_size, peer)],
            dst_ref=o_ref.at[part(concat, concat_size, me)],
            send_sem=send_sems.at[step - 1],
            recv_sem=recv_sems.at[step - 1],
            device_id={name: peer},
            device_id_type=MESH,
        )
        copy.start()
        copies.append(copy)
    own = pltpu.make_async_copy(
        x_ref.at[part(split, split_size, me)], o_ref.at[part(concat, concat_size, me)], own_sem
    )
    own.start()
    own.wait()
    for copy in copies:
        copy.wait()


def exchange(x, name, split, concat, ident):
    count = lax.axis_size(name)
    split_size = x.shape[split] // count
    concat_size = x.shape[concat]
    units = (1, 8, 128)
    if split_size % units[split] or concat_size % units[concat]:
        return lax.all_to_all(x, name, split_axis=split, concat_axis=concat, tiled=True)
    shape = list(x.shape)
    shape[split] = split_size
    shape[concat] = concat_size * count
    return pl.pallas_call(
        functools.partial(exchange_kernel, name, count, split, concat),
        out_shape=jax.ShapeDtypeStruct(tuple(shape), x.dtype),
        in_specs=[pl.BlockSpec(memory_space=pl.ANY)],
        out_specs=pl.BlockSpec(memory_space=pl.ANY),
        scratch_shapes=[
            pltpu.SemaphoreType.DMA,
            pltpu.SemaphoreType.DMA((count - 1,)),
            pltpu.SemaphoreType.DMA((count - 1,)),
        ],
        compiler_params=pltpu.CompilerParams(collective_id=ident, has_side_effects=True),
        name="exchange_" + name + str(ident),
    )(x)


def table_halves(x):
    high = lax.reduce_precision(x, 8, 7)
    return high.astype(jnp.bfloat16), (x - high).astype(jnp.bfloat16)


def halves(x):
    high = x.astype(jnp.bfloat16)
    low = (x - high.astype(jnp.float32)).astype(jnp.bfloat16)
    return high, low


def dot3(a, b, dims=(((1,), (0,)), ((), ()))):
    a_high, a_low = a
    b_high, b_low = b
    dot = functools.partial(lax.dot_general, dimension_numbers=dims, preferred_element_type=jnp.float32)
    return dot(a_high, b_high) + (dot(a_high, b_low) + dot(a_low, b_high))


def lateral_kernel(group, high_ref, low_ref, columns_ref, visc_ref, out_ref):
    table = (high_ref[...], low_ref[...])
    columns = jnp.concatenate([columns_ref[i] for i in range(group)], axis=1)
    physical = dot3(table, halves(columns))
    visc = jnp.concatenate([visc_ref[i].T for i in range(group)], axis=1)
    stress = visc * jnp.exp(jnp.log(1.0 + physical * physical) * (-1.0 / 3.0)) * physical
    back = dot3(table, halves(stress))
    width = back.shape[1] // group
    for i in range(group):
        out_ref[i] = back[:, i * width:(i + 1) * width]


def lateral_stage(table, columns, visc_base):
    depth, total_y, cells_x = columns.shape
    group = 2 if depth % 2 == 0 and cells_x % 128 == 0 else 1
    return pl.pallas_call(
        functools.partial(lateral_kernel, group),
        grid=(depth // group,),
        out_shape=jax.ShapeDtypeStruct(columns.shape, columns.dtype),
        in_specs=[
            pl.BlockSpec((total_y, total_y), lambda z: (0, 0)),
            pl.BlockSpec((total_y, total_y), lambda z: (0, 0)),
            pl.BlockSpec((group, total_y, cells_x), lambda z: (z, 0, 0)),
            pl.BlockSpec((group, cells_x, total_y), lambda z: (z, 0, 0)),
        ],
        out_specs=pl.BlockSpec((group, total_y, cells_x), lambda z: (z, 0, 0)),
        compiler_params=pltpu.CompilerParams(vmem_limit_bytes=VMEM_LIMIT),
        name="lateral_stage",
    )(*table, columns, visc_base)


def lines_kernel(high_ref, low_ref, x_ref, out_ref):
    out_ref[...] = dot3(halves(x_ref[...]), (high_ref[...], low_ref[...]))


def lines_stage(table, x):
    depth, rows, total = x.shape
    flat = x.reshape(depth * rows, total)
    tile = math.gcd(depth * rows, 256)
    out = pl.pallas_call(
        lines_kernel,
        grid=(depth * rows // tile,),
        out_shape=jax.ShapeDtypeStruct(flat.shape, flat.dtype),
        in_specs=[
            pl.BlockSpec((total, total), lambda i: (0, 0)),
            pl.BlockSpec((total, total), lambda i: (0, 0)),
            pl.BlockSpec((tile, total), lambda i: (i, 0)),
        ],
        out_specs=pl.BlockSpec((tile, total), lambda i: (i, 0)),
        compiler_params=pltpu.CompilerParams(vmem_limit_bytes=VMEM_LIMIT),
        name="lines_stage",
    )(*table, flat)
    return out.reshape(x.shape)


def local_plain(mode_field, forcing, visc_base, depth_inverse):
    depth_count = mode_field.shape[0]
    rows_y = mode_field.shape[1]
    cols_x = mode_field.shape[2]
    total_y = rows_y * lax.axis_size("px")
    total_x = cols_x * lax.axis_size("py")
    cell_total = depth_count * total_y * total_x
    forward, backward = depth_tables(depth_count)
    table_x = table_halves(hartley_table(total_x))
    table_y = table_halves(hartley_table(total_y))
    index_y = lax.axis_index("px") * rows_y + jnp.arange(rows_y, dtype=jnp.int32)
    index_x = lax.axis_index("py") * cols_x + jnp.arange(cols_x, dtype=jnp.int32)
    lateral = wave_square(index_y, total_y)[:, None] + wave_square(index_x, total_x)[None, :]
    field = mode_field
    partials = []
    for sweep in range(ITERS):
        points = jnp.einsum("jm,myx->jyx", forward, field, precision=HIGH)
        lines = exchange(points, "py", 0, 2, 0)
        lines = lines_stage(table_x, lines)
        columns = exchange(lines, "px", 2, 1, 1)
        returned = lateral_stage(table_y, columns, visc_base)
        returned = exchange(returned, "px", 1, 2, 2)
        returned = lines_stage(table_x, returned)
        spectral = exchange(returned, "py", 2, 0, 3)
        viscous = jnp.einsum("mj,jyx->myx", backward, spectral, precision=HIGH)
        residual = forcing - (lateral * field + viscous)
        squares = jnp.sum(residual * residual)
        partials.append(squares)
        correction = jnp.einsum("xmn,nyx->myx", depth_inverse, residual, precision=HIGH)
        field = field + correction / (1.0 + lateral)
    norm_values = lax.psum(jnp.stack(partials), ("px", "py")) / cell_total
    return (field, norm_values)


def hartley_factors(count, step):
    line = np.arange(count)
    coarse = 2.0 * np.pi * (np.arange(count // step)[:, None] * step * line[None, :] % count) / count
    fine = 2.0 * np.pi * (np.arange(step)[:, None] * line[None, :] % count) / count
    scale = 1.0 / np.sqrt(count)
    parts = (
        (np.cos(coarse) + np.sin(coarse)) * scale,
        (np.cos(coarse) - np.sin(coarse)) * scale,
        np.cos(fine),
        np.sin(fine),
    )
    return tuple(jnp.asarray(part, jnp.float32) for part in parts)


def depth_factors(count):
    index = np.arange(count)
    angle = np.pi * (index[:, None] * index[None, :] % (2 * (count - 1))) / (count - 1)
    ends = np.where((index == 0) | (index == count - 1), 2.0, 1.0)
    forward = np.cos(angle)
    backward = 2.0 / (count - 1) * np.cos(angle) / (ends[:, None] * ends[None, :])
    spread = np.stack([np.kron(table, np.eye(SUB)) for table in (forward, backward)]).astype(np.float32)
    high = spread.astype(jnp.bfloat16)
    low = (spread - high.astype(np.float32)).astype(jnp.bfloat16)
    return jnp.asarray(high), jnp.asarray(low)


FINE = 32
SUB = 8


def fused_kernel(
    sizes, field_hbm, forcing_hbm, visc_hbm, inverse_hbm, kron_high_hbm, kron_low_hbm, *rest,
):
    factors_hbm, (field, norm_ref), scratch = rest[:8], rest[8:10], rest[10:]
    (
        forcing, visc, inverse, tx_high, tx_low, ty_high, ty_low, kron_high, kron_low,
        send_p, lines, send_f, columns, send_b, returned, send_s, spectral,
        x_both, resid, correct, norm_sum, norm_send, norm_all,
        stage, load_sem, stage_sem, field_sem, kron_sem, factor_sem, p_send, p_recv, p_first, f_send, f_recv, b_send, b_recv, b_last, s_send, s_recv, n_send, n_recv,
        lateral_ref, scale_ref, *factors,
    ) = scratch
    P, Q, Z, RY, W, DL, XB, KC, C, DG, iters, cell_total = sizes
    i = lax.axis_index("px")
    q = lax.axis_index("py")
    groups = DL // DG
    early = min(C - 1, max(1, 16 // KC))
    pairs_per_group = DG // 2

    def remote(src, dst, send, recv, name, peer):
        pltpu.make_async_remote_copy(
            src_ref=src, dst_ref=dst, send_sem=send, recv_sem=recv,
            device_id={name: peer}, device_id_type=MESH,
        ).start()

    def local_copy(src, dst, sem):
        pltpu.make_async_copy(src, dst, sem).start()

    def wait_bytes(ref, sem):
        pltpu.make_async_copy(ref, ref, sem).wait()

    for c in range(C):
        rows = pl.ds(c * KC, KC)
        local_copy(field_hbm.at[:, rows], field.at[:, rows], field_sem.at[c])
        if c < 2:
            local_copy(kron_high_hbm.at[c], kron_high.at[c], kron_sem.at[2 * c])
            local_copy(kron_low_hbm.at[c], kron_low.at[c], kron_sem.at[2 * c + 1])

    for slot, (src, dst) in enumerate(zip(factors_hbm, factors)):
        local_copy(src, dst, factor_sem.at[slot])

    barrier = pltpu.get_barrier_semaphore()
    for step in range(1, P * Q):
        place = lax.rem(i * Q + q + step, P * Q)
        peer = {"px": place // Q, "py": lax.rem(place, Q)}
        pl.semaphore_signal(barrier, inc=1, device_id=peer, device_id_type=MESH)

    def make_table(p_ref, m_ref, c_ref, s_ref, store):
        cosine, sine = c_ref, s_ref

        def body(a, carry):
            plus = p_ref[pl.ds(a, 1), :]
            minus = m_ref[pl.ds(a, 1), :]
            high, low = halves(plus * cosine[...] + minus * sine[...])
            store(pl.multiple_of(a * FINE, FINE), high, low)
            return carry

        lax.fori_loop(0, p_ref.shape[0], body, 0)

    def store_x(start, high, low):
        for n in range(Q):
            tx_high[n, pl.ds(start, FINE), :] = high[:, n * W:(n + 1) * W]
            tx_low[n, pl.ds(start, FINE), :] = low[:, n * W:(n + 1) * W]

    def store_y(start, high, low):
        ty_high[pl.ds(start, FINE), :] = high
        ty_low[pl.ds(start, FINE), :] = low

    def kron_dot(which, x):
        return dot3((kron_high[which], kron_low[which]), halves(x.reshape(Z * SUB, W))).reshape(Z, SUB, W)

    def transform(count, store):
        def body(s, carry):
            n = lax.rem(q + Q // 2 + s, Q)
            both = jnp.dot(x_both[:2 * count], tx_high[n], preferred_element_type=jnp.float32)
            cross = jnp.dot(x_both[:count], tx_low[n], preferred_element_type=jnp.float32)
            store(n, both[:count] + (cross + both[count:]))
            return carry

        lax.fori_loop(0, Q, body, 0)

    def split(block, start, width):
        count = block.shape[0] * KC
        high, low = halves(block.reshape(count, width))
        x_both[:count, start:start + width] = high
        x_both[count:2 * count, start:start + width] = low

    def back_part(c, start, count):
        depths = pl.ds(start, count)
        for p in range(P):
            split(returned[c, p, depths], p * XB, XB)

        def store(n, value):
            send_s[c, n, depths] = value.reshape(count, KC, W)
            target = spectral.at[c, pl.ds(q * DL + start, count)]

            @pl.when(n != q)
            def _():
                remote(send_s.at[c, n, depths], target, s_send.at[c], s_recv.at[c], "py", n)

            @pl.when(n == q)
            def _():
                local_copy(send_s.at[c, n, depths], target, s_recv.at[c])

        transform(count * KC, store)

    def back_step(c):
        @pl.when(c < C - 1)
        def _():
            wait_bytes(returned.at[c], b_recv.at[c])
            back_part(c, 0, DL)

        @pl.when(c == C - 1)
        def _():
            def part(g, carry):
                wait_bytes(returned.at[c, :, pl.ds(g * DG, DG)], b_last.at[g])
                back_part(c, g * DG, DG)
                return carry

            lax.fori_loop(0, groups, part, 0)

        wait_bytes(send_f.at[c, pl.ds(0, P - 1)], f_send.at[c])

    def solve(c, turn):
        wait_bytes(spectral.at[c], s_recv.at[c])
        wait_bytes(send_s.at[c, pl.ds(0, Q - 1)], s_send.at[c])
        wait_bytes(returned.at[c, pl.ds(0, P - 1)], b_send.at[c])

        def residual(t, carry):
            at = pl.ds(pl.multiple_of(t * SUB, SUB), SUB)
            rows = pl.ds(pl.multiple_of(c * KC + t * SUB, SUB), SUB)
            viscous = kron_dot(1, spectral[c, :, at, :])
            value = forcing[:, rows, :] - (lateral_ref[rows, :][None] * field[:, rows, :] + viscous)
            resid[:, at, :] = value
            norm_sum[turn - 1] += jnp.sum(value * value, axis=0)
            return carry

        lax.fori_loop(0, KC // SUB, residual, 0)

        last = (turn == iters) & (c == C - 1)

        @pl.when(last)
        def _():
            total = norm_sum[...]
            norm_send[0] = sum(total[:, :, k * 128:(k + 1) * 128] for k in range(W // 128))
            mine = i * Q + q
            for step in range(1, P * Q):
                place = lax.rem(mine + step, P * Q)
                pltpu.make_async_remote_copy(
                    src_ref=norm_send.at[0], dst_ref=norm_all.at[mine], send_sem=n_send.at[0], recv_sem=n_recv.at[0],
                    device_id={"px": place // Q, "py": lax.rem(place, Q)}, device_id_type=MESH,
                ).start()
            local_copy(norm_send.at[0], norm_all.at[mine], n_recv.at[0])

        quads = SUB // 4

        def correction(b, carry):
            t = b // (W // 128)
            lane = pl.multiple_of(lax.rem(b, W // 128) * 128, 128)
            at = pl.ds(pl.multiple_of(t * SUB, SUB), SUB)
            for quad in range(quads):
                def body(n, sums):
                    mix = inverse[n, :, pl.ds(lane, 128)]
                    r = resid[n, at, pl.ds(lane, 128)]
                    return tuple(
                        total + mix * r[quad * 4 + k:quad * 4 + k + 1, :] for k, total in enumerate(sums)
                    )

                zero = jnp.zeros((Z, 128), jnp.float32)
                sums = lax.fori_loop(0, Z, body, (zero,) * 4, unroll=8)
                for k in range(4):
                    correct[t, quad * 4 + k, :, pl.ds(lane, 128)] = sums[k]
            return carry

        lax.fori_loop(0, KC // SUB * (W // 128), correction, 0)

        def update(u, carry):
            t = u // (Z // 8)
            m = pl.ds(pl.multiple_of(lax.rem(u, Z // 8) * 8, 8), 8)
            rows = pl.ds(pl.multiple_of(c * KC + t * SUB, SUB), SUB)
            value = jnp.swapaxes(correct[t, :, m, :], 0, 1)
            field[m, rows, :] += value * scale_ref[rows, :][None]
            return carry

        lax.fori_loop(0, KC // SUB * (Z // 8), update, 0)

    def points(c):
        def body(t, carry):
            at = pl.ds(pl.multiple_of(t * SUB, SUB), SUB)
            rows = pl.ds(pl.multiple_of(c * KC + t * SUB, SUB), SUB)
            send_p[c, :, at, :] = kron_dot(0, field[:, rows, :])
            return carry

        lax.fori_loop(0, KC // SUB, body, 0)

        def ship(start, count, recv):
            for step in range(1, Q):
                n = lax.rem(q + (Q // 2 + step - 1 if step <= Q - Q // 2 else step - (Q - Q // 2)), Q)
                part = send_p.at[c, pl.ds(n * DL + start, count)]
                remote(part, lines.at[c, q, pl.ds(start, count)], p_send.at[c], recv, "py", n)
            part = send_p.at[c, pl.ds(q * DL + start, count)]
            local_copy(part, lines.at[c, q, pl.ds(start, count)], recv)

        @pl.when(c > 0)
        def _():
            ship(0, DL, p_recv.at[c])

        @pl.when(c == 0)
        def _():
            def part(g, carry):
                ship(g * DG, DG, p_first.at[g])
                return carry

            lax.fori_loop(0, groups, part, 0)

    def line_part(c, start, count):
        depths = pl.ds(start, count)
        for n in range(Q):
            split(lines[c, n, depths], n * W, W)
        per = W // XB

        def store(n, value):
            for k in range(per):
                send_f[c, n * per + k, depths] = value[:, k * XB:(k + 1) * XB].reshape(count, KC, XB)

        transform(count * KC, store)

    def line_send(c, g):
        depths = pl.ds(g * DG, DG)
        mine = pl.ds(pl.multiple_of(i * RY + c * KC, SUB), KC)
        for step in range(1, P):
            peer = lax.rem(i + P // 2 + step - 1 if step <= P // 2 else i + step - P // 2, P)
            remote(send_f.at[c, peer, depths], columns.at[depths, mine], f_send.at[c], f_recv.at[g], "px", peer)
        local_copy(send_f.at[c, i, depths], columns.at[depths, mine], f_recv.at[g])

    def line_step(c):
        @pl.when(c > 0)
        def _():
            wait_bytes(lines.at[c], p_recv.at[c])
            line_part(c, 0, DL)

            def send(g, carry):
                line_send(c, g)
                return carry

            lax.fori_loop(0, groups, send, 0)

        @pl.when(c == 0)
        def _():
            def part(g, carry):
                wait_bytes(lines.at[c, :, pl.ds(g * DG, DG)], p_first.at[g])
                line_part(c, g * DG, DG)
                line_send(c, g)
                return carry

            lax.fori_loop(0, groups, part, 0)

        wait_bytes(send_p.at[c, pl.ds(0, Z - DL)], p_send.at[c])

    def send_back(c, depths, recv):
        for step in range(1, P):
            peer = lax.rem(i + P // 2 + step - 1 if step <= P // 2 else i + step - P // 2, P)
            rows = pl.ds(pl.multiple_of(peer * RY + c * KC, SUB), KC)
            remote(send_b.at[depths, rows], returned.at[c, i, depths], b_send.at[c], recv, "px", peer)
        rows = pl.ds(pl.multiple_of(i * RY + c * KC, SUB), KC)
        local_copy(send_b.at[depths, rows], returned.at[c, i, depths], recv)

    def lateral_step():
        def body(pair, carry):
            g = pair // pairs_per_group

            @pl.when(lax.rem(pair, pairs_per_group) == 0)
            def _():
                wait_bytes(columns.at[pl.ds(g * DG, DG)], f_recv.at[g])

            table = (ty_high[...], ty_low[...])
            block = jnp.concatenate([columns[2 * pair + k] for k in range(2)], axis=1)
            physical = dot3(table, halves(block))
            base = jnp.concatenate([visc[2 * pair + k].T for k in range(2)], axis=1)
            stress = base * jnp.exp(jnp.log(1.0 + physical * physical) * (-1.0 / 3.0)) * physical
            back = dot3(table, halves(stress))
            for k in range(2):
                send_b[2 * pair + k] = back[:, k * XB:(k + 1) * XB]

            @pl.when(lax.rem(pair, pairs_per_group) == pairs_per_group - 1)
            def _():
                for c in range(early):
                    send_back(c, pl.ds(g * DG, DG), b_recv.at[c])

            return carry

        lax.fori_loop(0, DL // 2, body, 0)

        def rest(c, carry):
            send_back(c, pl.ds(0, DL), b_recv.at[c])
            return carry

        lax.fori_loop(early, C - 1, rest, 0)

        def final(g, carry):
            send_back(C - 1, pl.ds(g * DG, DG), b_last.at[g])
            return carry

        lax.fori_loop(0, groups, final, 0)

    def make_lateral():
        y = wave_square(i * RY + lax.broadcasted_iota(jnp.int32, (RY, W), 0), RY * P)
        x = wave_square(q * W + lax.broadcasted_iota(jnp.int32, (RY, W), 1), W * Q)
        lateral_ref[...] = y + x
        scale_ref[...] = 1.0 / (1.0 + (y + x))

    def swap_inverse():
        def fetch(b, slot):
            block = pl.ds(pl.multiple_of(b * SUB, SUB), SUB)
            local_copy(inverse_hbm.at[block], stage.at[slot], stage_sem.at[slot])

        fetch(0, 0)

        def body(b, carry):
            slot = lax.rem(b, 2)
            wait_bytes(stage.at[slot], stage_sem.at[slot])

            @pl.when(b + 1 < Z // SUB)
            def _():
                fetch(b + 1, 1 - slot)

            m = pl.ds(pl.multiple_of(b * SUB, SUB), SUB)

            def swap(u, inner):
                n = pl.ds(pl.multiple_of(u * SUB, SUB), SUB)
                inverse[n, m, :] = jnp.swapaxes(stage[slot, :, n, :], 0, 1)
                return inner

            return lax.fori_loop(0, Z // SUB, swap, carry)

        lax.fori_loop(0, Z // SUB, body, 0)

    norm_sum[...] = jnp.zeros_like(norm_sum)
    wait_bytes(kron_high.at[0], kron_sem.at[0])
    wait_bytes(kron_low.at[0], kron_sem.at[1])
    pl.semaphore_wait(barrier, P * Q - 1)

    def turn_body(turn, carry):
        def step(t, inner):
            @pl.when((turn > 0) & (t < C))
            def _():
                back_step(t)

            @pl.when((t >= 1) & (t <= C))
            def _():
                c = t - 1

                @pl.when(turn > 0)
                def _():
                    solve(c, turn)

                @pl.when(turn == 0)
                def _():
                    rows = pl.ds(pl.multiple_of(c * KC, SUB), KC)
                    wait_bytes(field.at[:, rows], field_sem.at[c])

                @pl.when(turn < iters)
                def _():
                    points(c)

            @pl.when((turn == 0) & (t == 1))
            def _():
                for slot, (src, dst) in enumerate(zip(factors_hbm, factors)):
                    wait_bytes(dst, factor_sem.at[slot])
                make_table(*factors[:4], store_x)
                local_copy(forcing_hbm, forcing, load_sem.at[0])
                local_copy(visc_hbm, visc, load_sem.at[1])

            @pl.when((turn < iters) & (t >= 2))
            def _():
                line_step(t - 2)

            return inner

        lax.fori_loop(0, C + 2, step, 0)

        @pl.when(turn == 0)
        def _():
            make_table(*factors[4:], store_y)
            wait_bytes(kron_high.at[1], kron_sem.at[2])
            wait_bytes(kron_low.at[1], kron_sem.at[3])
            make_lateral()
            swap_inverse()
            wait_bytes(forcing, load_sem.at[0])
            wait_bytes(visc, load_sem.at[1])

        @pl.when(turn < iters)
        def _():
            lateral_step()

        return carry

    lax.fori_loop(0, iters + 1, turn_body, 0)

    wait_bytes(norm_all, n_recv.at[0])
    wait_bytes(norm_all.at[pl.ds(0, P * Q - 1)], n_send.at[0])
    whole = jnp.sum(norm_all[...], axis=0)
    for k in range(iters):
        norm_ref[k] = jnp.sum(whole[k]) / cell_total


def fused_plan(shape, P, Q):
    Z, RY, W = shape
    NX = W * Q
    if Z % Q or NX % P or P < 2 or Q < 2 or Q % 2 or P % 2:
        return None
    DL, XB = Z // Q, NX // P
    KC = 8
    if RY % KC or XB % 128 or W % XB or DL % 4 or Z % 8 or NX % FINE or (RY * P) % FINE:
        return None
    arrays = 12 * Z * RY * W * 4 + NX * NX * 4 + (RY * P) ** 2 * 4 + (Z * SUB) ** 2 * 8
    arrays += DL * KC * NX * 4 + Z * KC * W * 8
    if arrays > 60 * 2**20:
        return None
    return (P, Q, Z, RY, W, DL, XB, KC, RY // KC, 4, ITERS)


def fused(plan, mode_field, forcing, visc_base, depth_inverse):
    P, Q, Z, RY, W, DL, XB, KC, C, DG, iters = plan
    NX, NY = W * Q, RY * P
    factors = hartley_factors(NX, FINE) + hartley_factors(NY, FINE)
    inverse = jnp.transpose(depth_inverse, (1, 2, 0))
    f32, bf16 = jnp.float32, jnp.bfloat16
    vmem = pl.BlockSpec(memory_space=pltpu.VMEM)
    anywhere = pl.BlockSpec(memory_space=pl.ANY)
    dma = pltpu.SemaphoreType.DMA
    out, norms = pl.pallas_call(
        functools.partial(fused_kernel, plan + (float(Z * NX * NY),)),
        out_shape=(
            pltpu.VMEM(mode_field.shape, f32),
            jax.ShapeDtypeStruct((iters,), f32),
        ),
        in_specs=[anywhere] * 14,
        out_specs=(vmem, pl.BlockSpec(memory_space=pltpu.SMEM)),
        scratch_shapes=[
            pltpu.VMEM((Z, RY, W), f32),
            pltpu.VMEM((DL, XB, NY), f32),
            pltpu.VMEM((Z, Z, W), f32),
            pltpu.VMEM((Q, NX, W), bf16),
            pltpu.VMEM((Q, NX, W), bf16),
            pltpu.VMEM((NY, NY), bf16),
            pltpu.VMEM((NY, NY), bf16),
            pltpu.VMEM((2, Z * SUB, Z * SUB), bf16),
            pltpu.VMEM((2, Z * SUB, Z * SUB), bf16),
            pltpu.VMEM((C, Z, KC, W), f32),
            pltpu.VMEM((C, Q, DL, KC, W), f32),
            pltpu.VMEM((C, P, DL, KC, XB), f32),
            pltpu.VMEM((DL, NY, XB), f32),
            pltpu.VMEM((DL, NY, XB), f32),
            pltpu.VMEM((C, P, DL, KC, XB), f32),
            pltpu.VMEM((C, Q, DL, KC, W), f32),
            pltpu.VMEM((C, Z, KC, W), f32),
            pltpu.VMEM((2 * DL * KC, NX), bf16),
            pltpu.VMEM((Z, KC, W), f32),
            pltpu.VMEM((KC // SUB, SUB, Z, W), f32),
            pltpu.VMEM((iters, SUB, W), f32),
            pltpu.VMEM((1, iters, SUB, 128), f32),
            pltpu.VMEM((P * Q, iters, SUB, 128), f32),
            pltpu.VMEM((2, SUB, Z, W), f32),
            dma((2,)), dma((2,)), dma((C,)), dma((4,)), dma((8,)),
            dma((C,)), dma((C,)), dma((DL // DG,)),
            dma((C,)), dma((DL // DG,)),
            dma((C,)), dma((C,)), dma((DL // DG,)),
            dma((C,)), dma((C,)),
            dma((1,)), dma((1,)),
            pltpu.VMEM((RY, W), f32),
            pltpu.VMEM((RY, W), f32),
            *(pltpu.VMEM(factor.shape, f32) for factor in factors),
        ],
        compiler_params=pltpu.CompilerParams(
            collective_id=7, has_side_effects=True, vmem_limit_bytes=59 * 1024 * 1024
        ),
        name="fused",
    )(
        mode_field, forcing, visc_base, inverse, *depth_factors(Z), *factors,
    )
    return out, norms


def local(mode_field, forcing, visc_base, depth_inverse):
    plan = fused_plan(mode_field.shape, lax.axis_size("px"), lax.axis_size("py"))
    if plan is None:
        return local_plain(mode_field, forcing, visc_base, depth_inverse)
    return fused(plan, mode_field, forcing, visc_base, depth_inverse)


def solution(mesh):
    placed = (P(None, "px", "py"), P(None, "px", "py"), P("py", "px", None), P("py", None, None))
    return jax.shard_map(
        local, mesh=mesh, in_specs=placed, out_specs=(P(None, "px", "py"), P()), check_vma=False
    )
```

```python
import functools
import math

import jax
import jax.numpy as jnp
import numpy as np
from jax import lax
from jax.experimental import pallas as pl
from jax.experimental.pallas import tpu as pltpu
from jax.sharding import PartitionSpec as P

ITERS = 2
MESH = pl.DeviceIdType.MESH
HIGH = lax.Precision.HIGH
VMEM_LIMIT = 60000 * 1024


def depth_tables(count):
    index = jnp.arange(count, dtype=jnp.float32)
    angle = jnp.pi * index[:, None] * index[None, :] / (count - 1)
    ends = jnp.where((index == 0) | (index == count - 1), 2.0, 1.0)
    forward = jnp.cos(angle)
    backward = 2.0 / (count - 1) * jnp.cos(angle) / (ends[:, None] * ends[None, :])
    return (forward, backward)


def hartley_table(count):
    index = jnp.arange(count, dtype=jnp.int32)
    phase = index[:, None] * index[None, :] % count
    angle = phase.astype(jnp.float32) * (2.0 * math.pi / count)
    return (jnp.cos(angle) + jnp.sin(angle)) / math.sqrt(count)


def wave_square(index, count):
    folded = jnp.minimum(index, count - index).astype(jnp.float32)
    scaled = 2.0 * jnp.pi * folded / count
    return scaled * scaled


def part(axis, size, index):
    if axis == 0:
        return (pl.ds(index * size, size),)
    start = pl.multiple_of(index * size, 128 if axis == 2 else 8)
    return (slice(None),) * axis + (pl.ds(start, size),)


def exchange_kernel(name, count, split, concat, x_ref, o_ref, own_sem, send_sems, recv_sems):
    me = lax.axis_index(name)
    split_size = x_ref.shape[split] // count
    concat_size = x_ref.shape[concat]
    barrier = pltpu.get_barrier_semaphore()
    for step in range(1, count):
        peer = lax.rem(me + step, count)
        pl.semaphore_signal(barrier, inc=1, device_id={name: peer}, device_id_type=MESH)
    pl.semaphore_wait(barrier, count - 1)
    copies = []
    for step in range(1, count):
        peer = lax.rem(me + step, count)
        copy = pltpu.make_async_remote_copy(
            src_ref=x_ref.at[part(split, split_size, peer)],
            dst_ref=o_ref.at[part(concat, concat_size, me)],
            send_sem=send_sems.at[step - 1],
            recv_sem=recv_sems.at[step - 1],
            device_id={name: peer},
            device_id_type=MESH,
        )
        copy.start()
        copies.append(copy)
    own = pltpu.make_async_copy(
        x_ref.at[part(split, split_size, me)], o_ref.at[part(concat, concat_size, me)], own_sem
    )
    own.start()
    own.wait()
    for copy in copies:
        copy.wait()


def exchange(x, name, split, concat, ident):
    count = lax.axis_size(name)
    split_size = x.shape[split] // count
    concat_size = x.shape[concat]
    units = (1, 8, 128)
    if split_size % units[split] or concat_size % units[concat]:
        return lax.all_to_all(x, name, split_axis=split, concat_axis=concat, tiled=True)
    shape = list(x.shape)
    shape[split] = split_size
    shape[concat] = concat_size * count
    return pl.pallas_call(
        functools.partial(exchange_kernel, name, count, split, concat),
        out_shape=jax.ShapeDtypeStruct(tuple(shape), x.dtype),
        in_specs=[pl.BlockSpec(memory_space=pl.ANY)],
        out_specs=pl.BlockSpec(memory_space=pl.ANY),
        scratch_shapes=[
            pltpu.SemaphoreType.DMA,
            pltpu.SemaphoreType.DMA((count - 1,)),
            pltpu.SemaphoreType.DMA((count - 1,)),
        ],
        compiler_params=pltpu.CompilerParams(collective_id=ident, has_side_effects=True),
        name="exchange_" + name + str(ident),
    )(x)


def table_halves(x):
    high = lax.reduce_precision(x, 8, 7)
    return high.astype(jnp.bfloat16), (x - high).astype(jnp.bfloat16)


def halves(x):
    high = x.astype(jnp.bfloat16)
    low = (x - high.astype(jnp.float32)).astype(jnp.bfloat16)
    return high, low


def dot3(a, b, dims=(((1,), (0,)), ((), ()))):
    a_high, a_low = a
    b_high, b_low = b
    dot = functools.partial(lax.dot_general, dimension_numbers=dims, preferred_element_type=jnp.float32)
    return dot(a_high, b_high) + (dot(a_high, b_low) + dot(a_low, b_high))


def lateral_kernel(group, high_ref, low_ref, columns_ref, visc_ref, out_ref):
    table = (high_ref[...], low_ref[...])
    columns = jnp.concatenate([columns_ref[i] for i in range(group)], axis=1)
    physical = dot3(table, halves(columns))
    visc = jnp.concatenate([visc_ref[i].T for i in range(group)], axis=1)
    stress = visc * jnp.exp(jnp.log(1.0 + physical * physical) * (-1.0 / 3.0)) * physical
    back = dot3(table, halves(stress))
    width = back.shape[1] // group
    for i in range(group):
        out_ref[i] = back[:, i * width:(i + 1) * width]


def lateral_stage(table, columns, visc_base):
    depth, total_y, cells_x = columns.shape
    group = 2 if depth % 2 == 0 and cells_x % 128 == 0 else 1
    return pl.pallas_call(
        functools.partial(lateral_kernel, group),
        grid=(depth // group,),
        out_shape=jax.ShapeDtypeStruct(columns.shape, columns.dtype),
        in_specs=[
            pl.BlockSpec((total_y, total_y), lambda z: (0, 0)),
            pl.BlockSpec((total_y, total_y), lambda z: (0, 0)),
            pl.BlockSpec((group, total_y, cells_x), lambda z: (z, 0, 0)),
            pl.BlockSpec((group, cells_x, total_y), lambda z: (z, 0, 0)),
        ],
        out_specs=pl.BlockSpec((group, total_y, cells_x), lambda z: (z, 0, 0)),
        compiler_params=pltpu.CompilerParams(vmem_limit_bytes=VMEM_LIMIT),
        name="lateral_stage",
    )(*table, columns, visc_base)


def lines_kernel(high_ref, low_ref, x_ref, out_ref):
    out_ref[...] = dot3(halves(x_ref[...]), (high_ref[...], low_ref[...]))


def lines_stage(table, x):
    depth, rows, total = x.shape
    flat = x.reshape(depth * rows, total)
    tile = math.gcd(depth * rows, 256)
    out = pl.pallas_call(
        lines_kernel,
        grid=(depth * rows // tile,),
        out_shape=jax.ShapeDtypeStruct(flat.shape, flat.dtype),
        in_specs=[
            pl.BlockSpec((total, total), lambda i: (0, 0)),
            pl.BlockSpec((total, total), lambda i: (0, 0)),
            pl.BlockSpec((tile, total), lambda i: (i, 0)),
        ],
        out_specs=pl.BlockSpec((tile, total), lambda i: (i, 0)),
        compiler_params=pltpu.CompilerParams(vmem_limit_bytes=VMEM_LIMIT),
        name="lines_stage",
    )(*table, flat)
    return out.reshape(x.shape)


def local_plain(mode_field, forcing, visc_base, depth_inverse):
    depth_count = mode_field.shape[0]
    rows_y = mode_field.shape[1]
    cols_x = mode_field.shape[2]
    total_y = rows_y * lax.axis_size("px")
    total_x = cols_x * lax.axis_size("py")
    cell_total = depth_count * total_y * total_x
    forward, backward = depth_tables(depth_count)
    table_x = table_halves(hartley_table(total_x))
    table_y = table_halves(hartley_table(total_y))
    index_y = lax.axis_index("px") * rows_y + jnp.arange(rows_y, dtype=jnp.int32)
    index_x = lax.axis_index("py") * cols_x + jnp.arange(cols_x, dtype=jnp.int32)
    lateral = wave_square(index_y, total_y)[:, None] + wave_square(index_x, total_x)[None, :]
    field = mode_field
    partials = []
    for sweep in range(ITERS):
        points = jnp.einsum("jm,myx->jyx", forward, field, precision=HIGH)
        lines = exchange(points, "py", 0, 2, 0)
        lines = lines_stage(table_x, lines)
        columns = exchange(lines, "px", 2, 1, 1)
        returned = lateral_stage(table_y, columns, visc_base)
        returned = exchange(returned, "px", 1, 2, 2)
        returned = lines_stage(table_x, returned)
        spectral = exchange(returned, "py", 2, 0, 3)
        viscous = jnp.einsum("mj,jyx->myx", backward, spectral, precision=HIGH)
        residual = forcing - (lateral * field + viscous)
        squares = jnp.sum(residual * residual)
        partials.append(squares)
        correction = jnp.einsum("xmn,nyx->myx", depth_inverse, residual, precision=HIGH)
        field = field + correction / (1.0 + lateral)
    norm_values = lax.psum(jnp.stack(partials), ("px", "py")) / cell_total
    return (field, norm_values)


def hartley_factors(count, step):
    line = np.arange(count)
    coarse = 2.0 * np.pi * (np.arange(count // step)[:, None] * step * line[None, :] % count) / count
    fine = 2.0 * np.pi * (np.arange(step)[:, None] * line[None, :] % count) / count
    scale = 1.0 / np.sqrt(count)
    parts = (
        (np.cos(coarse) + np.sin(coarse)) * scale,
        (np.cos(coarse) - np.sin(coarse)) * scale,
        np.cos(fine),
        np.sin(fine),
    )
    return tuple(jnp.asarray(part, jnp.float32) for part in parts)


def depth_factors(count):
    index = np.arange(count)
    angle = np.pi * (index[:, None] * index[None, :] % (2 * (count - 1))) / (count - 1)
    ends = np.where((index == 0) | (index == count - 1), 2.0, 1.0)
    forward = np.cos(angle)
    backward = 2.0 / (count - 1) * np.cos(angle) / (ends[:, None] * ends[None, :])
    spread = np.stack([np.kron(table, np.eye(SUB)) for table in (forward, backward)]).astype(np.float32)
    high = spread.astype(jnp.bfloat16)
    low = (spread - high.astype(np.float32)).astype(jnp.bfloat16)
    return jnp.asarray(high), jnp.asarray(low)


FINE = 32
SUB = 8


def fused_kernel(
    sizes, field_hbm, forcing_hbm, visc_hbm, inverse_hbm, kron_high_hbm, kron_low_hbm, *rest,
):
    factors_hbm, (field, norm_ref), scratch = rest[:8], rest[8:10], rest[10:]
    (
        forcing, visc, inverse, tx_high, tx_low, ty_high, ty_low, kron_high, kron_low,
        send_p, lines, send_f, columns, send_b, returned, send_s, spectral,
        x_both, resid, correct, norm_sum, norm_send, norm_all,
        stage, load_sem, stage_sem, field_sem, kron_sem, factor_sem, p_send, p_recv, p_first, f_send, f_recv, b_send, b_recv, b_last, s_send, s_recv, n_send, n_recv,
        lateral_ref, scale_ref, *factors,
    ) = scratch
    P, Q, Z, RY, W, DL, XB, KC, C, DG, iters, cell_total = sizes
    i = lax.axis_index("px")
    q = lax.axis_index("py")
    groups = DL // DG
    early = min(C - 1, max(1, 16 // KC))
    pairs_per_group = DG // 2

    def remote(src, dst, send, recv, name, peer):
        pltpu.make_async_remote_copy(
            src_ref=src, dst_ref=dst, send_sem=send, recv_sem=recv,
            device_id={name: peer}, device_id_type=MESH,
        ).start()

    def local_copy(src, dst, sem):
        pltpu.make_async_copy(src, dst, sem).start()

    def wait_bytes(ref, sem):
        pltpu.make_async_copy(ref, ref, sem).wait()

    for c in range(C):
        rows = pl.ds(c * KC, KC)
        local_copy(field_hbm.at[:, rows], field.at[:, rows], field_sem.at[c])
        if c < 2:
            local_copy(kron_high_hbm.at[c], kron_high.at[c], kron_sem.at[2 * c])
            local_copy(kron_low_hbm.at[c], kron_low.at[c], kron_sem.at[2 * c + 1])

    for slot, (src, dst) in enumerate(zip(factors_hbm, factors)):
        local_copy(src, dst, factor_sem.at[slot])

    barrier = pltpu.get_barrier_semaphore()
    for step in range(1, P * Q):
        place = lax.rem(i * Q + q + step, P * Q)
        peer = {"px": place // Q, "py": lax.rem(place, Q)}
        pl.semaphore_signal(barrier, inc=1, device_id=peer, device_id_type=MESH)

    def make_table(p_ref, m_ref, c_ref, s_ref, store):
        cosine, sine = c_ref, s_ref

        def body(a, carry):
            plus = p_ref[pl.ds(a, 1), :]
            minus = m_ref[pl.ds(a, 1), :]
            high, low = halves(plus * cosine[...] + minus * sine[...])
            store(pl.multiple_of(a * FINE, FINE), high, low)
            return carry

        lax.fori_loop(0, p_ref.shape[0], body, 0, unroll=4)

    def store_x(start, high, low):
        for n in range(Q):
            tx_high[n, pl.ds(start, FINE), :] = high[:, n * W:(n + 1) * W]
            tx_low[n, pl.ds(start, FINE), :] = low[:, n * W:(n + 1) * W]

    def store_y(start, high, low):
        ty_high[pl.ds(start, FINE), :] = high
        ty_low[pl.ds(start, FINE), :] = low

    def kron_dot(which, x):
        return dot3((kron_high[which], kron_low[which]), halves(x.reshape(Z * SUB, W))).reshape(Z, SUB, W)

    def transform(count, store):
        def body(s, carry):
            n = lax.rem(q + Q // 2 + s, Q)
            both = jnp.dot(x_both[:2 * count], tx_high[n], preferred_element_type=jnp.float32)
            cross = jnp.dot(x_both[:count], tx_low[n], preferred_element_type=jnp.float32)
            store(n, both[:count] + (cross + both[count:]))
            return carry

        lax.fori_loop(0, Q, body, 0)

    def split(block, start, width):
        count = block.shape[0] * KC
        high, low = halves(block.reshape(count, width))
        x_both[:count, start:start + width] = high
        x_both[count:2 * count, start:start + width] = low

    def back_part(c, start, count):
        depths = pl.ds(start, count)
        for p in range(P):
            split(returned[c, p, depths], p * XB, XB)

        def store(n, value):
            send_s[c, n, depths] = value.reshape(count, KC, W)
            target = spectral.at[c, pl.ds(q * DL + start, count)]

            @pl.when(n != q)
            def _():
                remote(send_s.at[c, n, depths], target, s_send.at[c], s_recv.at[c], "py", n)

            @pl.when(n == q)
            def _():
                local_copy(send_s.at[c, n, depths], target, s_recv.at[c])

        transform(count * KC, store)

    def back_step(c):
        @pl.when(c < C - 1)
        def _():
            wait_bytes(returned.at[c], b_recv.at[c])
            back_part(c, 0, DL)

        @pl.when(c == C - 1)
        def _():
            def part(g, carry):
                wait_bytes(returned.at[c, :, pl.ds(2 * g * DG, DG)], b_last.at[2 * g])
                wait_bytes(returned.at[c, :, pl.ds(2 * g * DG + DG, DG)], b_last.at[2 * g + 1])
                back_part(c, 2 * g * DG, 2 * DG)
                return carry

            lax.fori_loop(0, groups // 2, part, 0)

        wait_bytes(send_f.at[c, pl.ds(0, P - 1)], f_send.at[c])

    def solve(c, turn):
        wait_bytes(spectral.at[c], s_recv.at[c])
        wait_bytes(send_s.at[c, pl.ds(0, Q - 1)], s_send.at[c])
        wait_bytes(returned.at[c, pl.ds(0, P - 1)], b_send.at[c])

        def residual(t, carry):
            at = pl.ds(pl.multiple_of(t * SUB, SUB), SUB)
            rows = pl.ds(pl.multiple_of(c * KC + t * SUB, SUB), SUB)
            viscous = kron_dot(1, spectral[c, :, at, :])
            value = forcing[:, rows, :] - (lateral_ref[rows, :][None] * field[:, rows, :] + viscous)
            resid[:, at, :] = value
            norm_sum[turn - 1] += jnp.sum(value * value, axis=0)
            return carry

        lax.fori_loop(0, KC // SUB, residual, 0)

        last = (turn == iters) & (c == C - 1)

        @pl.when(last)
        def _():
            total = norm_sum[...]
            norm_send[0] = sum(total[:, :, k * 128:(k + 1) * 128] for k in range(W // 128))
            mine = i * Q + q
            for step in range(1, P * Q):
                place = lax.rem(mine + step, P * Q)
                pltpu.make_async_remote_copy(
                    src_ref=norm_send.at[0], dst_ref=norm_all.at[mine], send_sem=n_send.at[0], recv_sem=n_recv.at[0],
                    device_id={"px": place // Q, "py": lax.rem(place, Q)}, device_id_type=MESH,
                ).start()
            local_copy(norm_send.at[0], norm_all.at[mine], n_recv.at[0])

        quads = SUB // 4

        def correction(b, carry):
            t = b // (W // 128)
            lane = pl.multiple_of(lax.rem(b, W // 128) * 128, 128)
            at = pl.ds(pl.multiple_of(t * SUB, SUB), SUB)
            for quad in range(quads):
                def body(n, sums):
                    mix = inverse[n, :, pl.ds(lane, 128)]
                    r = resid[n, at, pl.ds(lane, 128)]
                    return tuple(
                        total + mix * r[quad * 4 + k:quad * 4 + k + 1, :] for k, total in enumerate(sums)
                    )

                zero = jnp.zeros((Z, 128), jnp.float32)
                sums = lax.fori_loop(0, Z, body, (zero,) * 4, unroll=8)
                for k in range(4):
                    correct[t, quad * 4 + k, :, pl.ds(lane, 128)] = sums[k]
            return carry

        lax.fori_loop(0, KC // SUB * (W // 128), correction, 0)

        def update(u, carry):
            t = u // (Z // 8)
            m = pl.ds(pl.multiple_of(lax.rem(u, Z // 8) * 8, 8), 8)
            rows = pl.ds(pl.multiple_of(c * KC + t * SUB, SUB), SUB)
            value = jnp.swapaxes(correct[t, :, m, :], 0, 1)
            field[m, rows, :] += value * scale_ref[rows, :][None]
            return carry

        lax.fori_loop(0, KC // SUB * (Z // 8), update, 0)

    def points(c):
        def body(t, carry):
            at = pl.ds(pl.multiple_of(t * SUB, SUB), SUB)
            rows = pl.ds(pl.multiple_of(c * KC + t * SUB, SUB), SUB)
            send_p[c, :, at, :] = kron_dot(0, field[:, rows, :])
            return carry

        lax.fori_loop(0, KC // SUB, body, 0)

        def ship(start, count, recv):
            for step in range(1, Q):
                n = lax.rem(q + (Q // 2 + step - 1 if step <= Q - Q // 2 else step - (Q - Q // 2)), Q)
                part = send_p.at[c, pl.ds(n * DL + start, count)]
                remote(part, lines.at[c, q, pl.ds(start, count)], p_send.at[c], recv, "py", n)
            part = send_p.at[c, pl.ds(q * DL + start, count)]
            local_copy(part, lines.at[c, q, pl.ds(start, count)], recv)

        @pl.when(c > 0)
        def _():
            ship(0, DL, p_recv.at[c])

        @pl.when(c == 0)
        def _():
            def part(g, carry):
                ship(g * DG, DG, p_first.at[g])
                return carry

            lax.fori_loop(0, groups, part, 0)

    def line_part(c, start, count):
        depths = pl.ds(start, count)
        for n in range(Q):
            split(lines[c, n, depths], n * W, W)
        per = W // XB

        def store(n, value):
            for k in range(per):
                send_f[c, n * per + k, depths] = value[:, k * XB:(k + 1) * XB].reshape(count, KC, XB)

        transform(count * KC, store)

    def line_send(c, g):
        depths = pl.ds(g * DG, DG)
        mine = pl.ds(pl.multiple_of(i * RY + c * KC, SUB), KC)
        for step in range(1, P):
            peer = lax.rem(i + P // 2 + step - 1 if step <= P // 2 else i + step - P // 2, P)
            remote(send_f.at[c, peer, depths], columns.at[depths, mine], f_send.at[c], f_recv.at[g], "px", peer)
        local_copy(send_f.at[c, i, depths], columns.at[depths, mine], f_recv.at[g])

    def line_step(c):
        @pl.when(c > 0)
        def _():
            wait_bytes(lines.at[c], p_recv.at[c])
            line_part(c, 0, DL)

            def send(g, carry):
                line_send(c, g)
                return carry

            lax.fori_loop(0, groups, send, 0)

        @pl.when(c == 0)
        def _():
            def part(g, carry):
                wait_bytes(lines.at[c, :, pl.ds(g * DG, DG)], p_first.at[g])
                line_part(c, g * DG, DG)
                line_send(c, g)
                return carry

            lax.fori_loop(0, groups, part, 0)

        wait_bytes(send_p.at[c, pl.ds(0, Z - DL)], p_send.at[c])

    def send_back(c, depths, recv):
        for step in range(1, P):
            peer = lax.rem(i + P // 2 + step - 1 if step <= P // 2 else i + step - P // 2, P)
            rows = pl.ds(pl.multiple_of(peer * RY + c * KC, SUB), KC)
            remote(send_b.at[depths, rows], returned.at[c, i, depths], b_send.at[c], recv, "px", peer)
        rows = pl.ds(pl.multiple_of(i * RY + c * KC, SUB), KC)
        local_copy(send_b.at[depths, rows], returned.at[c, i, depths], recv)

    def lateral_step():
        def body(pair, carry):
            g = pair // pairs_per_group

            @pl.when(lax.rem(pair, pairs_per_group) == 0)
            def _():
                wait_bytes(columns.at[pl.ds(g * DG, DG)], f_recv.at[g])

            table = (ty_high[...], ty_low[...])
            block = jnp.concatenate([columns[2 * pair + k] for k in range(2)], axis=1)
            physical = dot3(table, halves(block))
            base = jnp.concatenate([visc[2 * pair + k].T for k in range(2)], axis=1)
            stress = base * jnp.exp(jnp.log(1.0 + physical * physical) * (-1.0 / 3.0)) * physical
            back = dot3(table, halves(stress))
            for k in range(2):
                send_b[2 * pair + k] = back[:, k * XB:(k + 1) * XB]

            @pl.when(lax.rem(pair, pairs_per_group) == pairs_per_group - 1)
            def _():
                for c in range(early):
                    send_back(c, pl.ds(g * DG, DG), b_recv.at[c])

            return carry

        lax.fori_loop(0, DL // 2, body, 0)

        def rest(c, carry):
            send_back(c, pl.ds(0, DL), b_recv.at[c])
            return carry

        lax.fori_loop(early, C - 1, rest, 0)

        def final(g, carry):
            send_back(C - 1, pl.ds(g * DG, DG), b_last.at[g])
            return carry

        lax.fori_loop(0, groups, final, 0)

    def make_lateral():
        y = wave_square(i * RY + lax.broadcasted_iota(jnp.int32, (RY, W), 0), RY * P)
        x = wave_square(q * W + lax.broadcasted_iota(jnp.int32, (RY, W), 1), W * Q)
        lateral_ref[...] = y + x
        scale_ref[...] = 1.0 / (1.0 + (y + x))

    def swap_inverse():
        def fetch(b, slot):
            block = pl.ds(pl.multiple_of(b * SUB, SUB), SUB)
            local_copy(inverse_hbm.at[block], stage.at[slot], stage_sem.at[slot])

        fetch(0, 0)

        def body(b, carry):
            slot = lax.rem(b, 2)
            wait_bytes(stage.at[slot], stage_sem.at[slot])

            @pl.when(b + 1 < Z // SUB)
            def _():
                fetch(b + 1, 1 - slot)

            m = pl.ds(pl.multiple_of(b * SUB, SUB), SUB)

            def swap(u, inner):
                n = pl.ds(pl.multiple_of(u * SUB, SUB), SUB)
                inverse[n, m, :] = jnp.swapaxes(stage[slot, :, n, :], 0, 1)
                return inner

            return lax.fori_loop(0, Z // SUB, swap, carry)

        lax.fori_loop(0, Z // SUB, body, 0)

    norm_sum[...] = jnp.zeros_like(norm_sum)
    wait_bytes(kron_high.at[0], kron_sem.at[0])
    wait_bytes(kron_low.at[0], kron_sem.at[1])
    pl.semaphore_wait(barrier, P * Q - 1)

    def turn_body(turn, carry):
        def step(t, inner):
            @pl.when((turn > 0) & (t < C))
            def _():
                back_step(t)

            @pl.when((t >= 1) & (t <= C))
            def _():
                c = t - 1

                @pl.when(turn > 0)
                def _():
                    solve(c, turn)

                @pl.when(turn == 0)
                def _():
                    rows = pl.ds(pl.multiple_of(c * KC, SUB), KC)
                    wait_bytes(field.at[:, rows], field_sem.at[c])

                @pl.when(turn < iters)
                def _():
                    points(c)

            @pl.when((turn == 0) & (t == 1))
            def _():
                for slot, (src, dst) in enumerate(zip(factors_hbm, factors)):
                    wait_bytes(dst, factor_sem.at[slot])
                make_table(*factors[:4], store_x)
                local_copy(forcing_hbm, forcing, load_sem.at[0])
                local_copy(visc_hbm, visc, load_sem.at[1])

            @pl.when((turn < iters) & (t >= 2))
            def _():
                line_step(t - 2)

            return inner

        lax.fori_loop(0, C + 2, step, 0)

        @pl.when(turn == 0)
        def _():
            make_table(*factors[4:], store_y)
            wait_bytes(kron_high.at[1], kron_sem.at[2])
            wait_bytes(kron_low.at[1], kron_sem.at[3])
            make_lateral()
            swap_inverse()
            wait_bytes(forcing, load_sem.at[0])
            wait_bytes(visc, load_sem.at[1])

        @pl.when(turn < iters)
        def _():
            lateral_step()

        return carry

    lax.fori_loop(0, iters + 1, turn_body, 0)

    wait_bytes(norm_all, n_recv.at[0])
    wait_bytes(norm_all.at[pl.ds(0, P * Q - 1)], n_send.at[0])
    whole = jnp.sum(norm_all[...], axis=0)
    for k in range(iters):
        norm_ref[k] = jnp.sum(whole[k]) / cell_total


def fused_plan(shape, P, Q):
    Z, RY, W = shape
    NX = W * Q
    if Z % Q or NX % P or P < 2 or Q < 2 or Q % 2 or P % 2:
        return None
    DL, XB = Z // Q, NX // P
    KC = 8
    if RY % KC or XB % 128 or W % XB or DL % 4 or Z % 8 or NX % FINE or (RY * P) % FINE:
        return None
    arrays = 12 * Z * RY * W * 4 + NX * NX * 4 + (RY * P) ** 2 * 4 + (Z * SUB) ** 2 * 8
    arrays += DL * KC * NX * 4 + Z * KC * W * 8
    if arrays > 60 * 2**20:
        return None
    return (P, Q, Z, RY, W, DL, XB, KC, RY // KC, 4, ITERS)


def fused(plan, mode_field, forcing, visc_base, depth_inverse):
    P, Q, Z, RY, W, DL, XB, KC, C, DG, iters = plan
    NX, NY = W * Q, RY * P
    factors = hartley_factors(NX, FINE) + hartley_factors(NY, FINE)
    inverse = jnp.transpose(depth_inverse, (1, 2, 0))
    f32, bf16 = jnp.float32, jnp.bfloat16
    vmem = pl.BlockSpec(memory_space=pltpu.VMEM)
    anywhere = pl.BlockSpec(memory_space=pl.ANY)
    dma = pltpu.SemaphoreType.DMA
    out, norms = pl.pallas_call(
        functools.partial(fused_kernel, plan + (float(Z * NX * NY),)),
        out_shape=(
            pltpu.VMEM(mode_field.shape, f32),
            jax.ShapeDtypeStruct((iters,), f32),
        ),
        in_specs=[anywhere] * 14,
        out_specs=(vmem, pl.BlockSpec(memory_space=pltpu.SMEM)),
        scratch_shapes=[
            pltpu.VMEM((Z, RY, W), f32),
            pltpu.VMEM((DL, XB, NY), f32),
            pltpu.VMEM((Z, Z, W), f32),
            pltpu.VMEM((Q, NX, W), bf16),
            pltpu.VMEM((Q, NX, W), bf16),
            pltpu.VMEM((NY, NY), bf16),
            pltpu.VMEM((NY, NY), bf16),
            pltpu.VMEM((2, Z * SUB, Z * SUB), bf16),
            pltpu.VMEM((2, Z * SUB, Z * SUB), bf16),
            pltpu.VMEM((C, Z, KC, W), f32),
            pltpu.VMEM((C, Q, DL, KC, W), f32),
            pltpu.VMEM((C, P, DL, KC, XB), f32),
            pltpu.VMEM((DL, NY, XB), f32),
            pltpu.VMEM((DL, NY, XB), f32),
            pltpu.VMEM((C, P, DL, KC, XB), f32),
            pltpu.VMEM((C, Q, DL, KC, W), f32),
            pltpu.VMEM((C, Z, KC, W), f32),
            pltpu.VMEM((2 * DL * KC, NX), bf16),
            pltpu.VMEM((Z, KC, W), f32),
            pltpu.VMEM((KC // SUB, SUB, Z, W), f32),
            pltpu.VMEM((iters, SUB, W), f32),
            pltpu.VMEM((1, iters, SUB, 128), f32),
            pltpu.VMEM((P * Q, iters, SUB, 128), f32),
            pltpu.VMEM((2, SUB, Z, W), f32),
            dma((2,)), dma((2,)), dma((C,)), dma((4,)), dma((8,)),
            dma((C,)), dma((C,)), dma((DL // DG,)),
            dma((C,)), dma((DL // DG,)),
            dma((C,)), dma((C,)), dma((DL // DG,)),
            dma((C,)), dma((C,)),
            dma((1,)), dma((1,)),
            pltpu.VMEM((RY, W), f32),
            pltpu.VMEM((RY, W), f32),
            *(pltpu.VMEM(factor.shape, f32) for factor in factors),
        ],
        compiler_params=pltpu.CompilerParams(
            collective_id=7, has_side_effects=True, vmem_limit_bytes=59 * 1024 * 1024
        ),
        name="fused",
    )(
        mode_field, forcing, visc_base, inverse, *depth_factors(Z), *factors,
    )
    return out, norms


def local(mode_field, forcing, visc_base, depth_inverse):
    plan = fused_plan(mode_field.shape, lax.axis_size("px"), lax.axis_size("py"))
    if plan is None:
        return local_plain(mode_field, forcing, visc_base, depth_inverse)
    return fused(plan, mode_field, forcing, visc_base, depth_inverse)


def solution(mesh):
    placed = (P(None, "px", "py"), P(None, "px", "py"), P("py", "px", None), P("py", None, None))
    return jax.shard_map(
        local, mesh=mesh, in_specs=placed, out_specs=(P(None, "px", "py"), P()), check_vma=False
    )
```
